512 devices in a mesh: batch: 128 (over x, y_lo, z), mp: 4 (over y_hi, core).
Axes of the slice: x: 4, y: 8 (y_hi: 2, y_lo: 4; y = y_hi * 4 + y_lo), z: 8, core: 2. Of those that a mesh axis runs over, the one named last changes fastest.
Arguments:
- img_feat: bfloat16 [2048, 1536], P('batch'), may hold values from -6 to 6
- txt_feat: bfloat16 [2048, 1536], P('batch'), may hold values from -6 to 6
- w_img: bfloat16 [1536, 1152], P('batch', 'mp'), may hold values from -0.15625 to 0.15625
- w_txt: bfloat16 [1536, 1152], P('batch', 'mp'), may hold values from -0.15625 to 0.15625
- pair_index: int32 [2048], P('batch'), may hold values from 0 to 2047, each once
- log_scale: float32 [1], replicated, may hold values from 2 to 2.6
- bias: float32 [1], replicated, may hold values from -6 to -4
Outputs:
- image_grad: float32 [2048, 1152], P('batch', 'mp')
- text_grad: float32 [2048, 1152], P(('batch', 'mp'))
The draws below stay inside these ranges and needn't reach their ends.
Inputs may be any that keep to these rules, and one draw needn't show every extreme that they name: `pair_index`: each text index appears exactly once.
All inputs are finite; a program needn't handle non-finite values.
Results may differ from the reference program's by a relative error of at most 0.0046.
Values may be sent and summed in bfloat16 or wider, within the bound.
No kernel may reach another device: no remote copies, remote signals or barrier semaphores. Data moves between devices by JAX's collectives and lax.ppermute only.
A program may use at most 64 MiB of HBM per device.

```python
import jax
import jax.numpy as jnp
from jax import lax

D = 1536
E = 1152
B_LOC = 16
B_TOT = 2048
N_BATCH = 128


def level_of(own_key, dims, pieces, least, top_value):
    factor_of = 1.0
    for position, blocks in pieces:
        heights = jax.random.uniform(jax.random.fold_in(jax.random.fold_in(own_key, 6), position), (blocks,), jnp.float32, least / len(pieces), top_value / len(pieces))
        factor_of = factor_of * jnp.repeat(jnp.exp(heights), dims[position] // blocks).reshape((-1,) + (1,) * (len(dims) - 1 - position))
    return factor_of


def gaussian(own_key, dims, width, most, cuts=(), kind=jnp.bfloat16):
    entries = jax.random.normal(own_key, dims, jnp.float32) * width
    if len(cuts) > 0:
        entries = level_of(own_key, dims, cuts, -0.22, 0.18) * entries
    return jnp.clip(entries, min=-most, max=most).astype(kind)


def setup_inputs(seed: int = 0) -> dict:
    key_list = jax.random.split(jax.random.key(seed), 8)
    return {
        "img_feat": gaussian(key_list[0], (B_TOT, D), 1.0, 6.0, ((0, 128),)),
        "txt_feat": gaussian(key_list[1], (B_TOT, D), 1.0, 6.0, ((0, 128),)),
        "w_img": gaussian(key_list[2], (D, E), D ** -0.5, 0.15625, ((0, 128), (1, 4))),
        "w_txt": gaussian(key_list[3], (D, E), D ** -0.5, 0.15625, ((0, 128), (1, 4))),
        "pair_index": jax.random.permutation(key_list[4], B_TOT).astype(jnp.int32),
        "log_scale": jnp.clip(jax.random.uniform(key_list[5], (1,), jnp.float32, 2.0, 2.6), 2.0, 2.6),
        "bias": jnp.clip(jax.random.uniform(key_list[6], (1,), jnp.float32, -6.0, -4.0), -6.0, -4.0),
    }


epsilon = 1e-06

def embed(feat, weight):
    pre = jnp.dot(feat, weight, preferred_element_type=jnp.float32).astype(jnp.bfloat16)
    values = pre.astype(jnp.float32)
    norm = lax.rsqrt(lax.optimization_barrier(jnp.sum(values * values, axis=1, keepdims=True)) + epsilon)
    return (values * norm).astype(jnp.bfloat16)

def reference(img_feat, txt_feat, w_img, w_txt, pair_index, log_scale, bias):
    image = embed(img_feat, w_img)
    text = embed(txt_feat, w_txt)
    scale = jnp.exp(log_scale[0])
    offset = bias[0]
    span = min(N_BATCH, 32)
    half = span // 2
    img_blocks = image.reshape(N_BATCH, B_LOC, E).astype(jnp.float32)
    txt_blocks = text.reshape(N_BATCH, B_LOC, E).astype(jnp.float32)
    pairing = pair_index.reshape(N_BATCH, B_LOC)
    block_ids = jnp.arange(N_BATCH, dtype=jnp.int32)
    inside = jnp.arange(B_LOC, dtype=jnp.int32)
    highest = lax.Precision.HIGHEST

    def one_offset(carry, step):
        img_total, txt_total = carry
        partner = jnp.roll(txt_blocks, -step, axis=0)
        scores = jnp.einsum('hie,hje->hij', img_blocks, partner, precision=highest)
        logits = scale * scores + offset
        columns = ((block_ids + step) % N_BATCH * B_LOC).astype(jnp.int32)[:, None] + inside[None, :]
        label = jnp.where(pairing[:, :, None] == columns[:, None, :], 1.0, -1.0).astype(jnp.float32)
        coef = (-label * jax.nn.sigmoid(-label * logits)).astype(jnp.bfloat16).astype(jnp.float32)
        img_total = img_total + jnp.einsum('hij,hje->hie', coef, partner, precision=highest)
        back = jnp.einsum('hij,hie->hje', coef, img_blocks, precision=highest)
        txt_total = txt_total + jnp.roll(back, step, axis=0)
        return ((img_total, txt_total), None)
    zeros = jnp.zeros((N_BATCH, B_LOC, E), jnp.float32)
    steps = jnp.arange(-half + 1, half + 1, dtype=jnp.int32)
    (img_total, txt_total), unused = lax.scan(one_offset, (zeros, zeros), steps)
    image_grad = scale * img_total.reshape(B_TOT, E)
    text_grad = scale * txt_total.reshape(B_TOT, E)
    return (image_grad, text_grad)
```

```python
import jax
import jax.numpy as jnp
from jax import lax
from jax.experimental import pallas as pl
from jax.experimental.pallas import tpu as pltpu
from jax.sharding import Mesh
from jax.sharding import PartitionSpec as P

BATCH = ("x", "y", "z")
MP = ("m0", "m1")
bf16 = jnp.bfloat16
f32 = jnp.float32
epsilon = 1e-06
DELTA = (-2, -1, 1, 2)


def call(body, out_shape, scratch, *args, smem=()):
    specs = [
        pl.BlockSpec(memory_space=pltpu.SMEM if k in smem else pltpu.VMEM)
        for k in range(len(args))
    ]
    outs = jax.tree.map(lambda _: pl.BlockSpec(memory_space=pltpu.VMEM), out_shape)
    return pl.pallas_call(
        body, out_shape=out_shape, in_specs=specs, out_specs=outs, scratch_shapes=scratch
    )(*args)


def project(w_ref, left_ref, own_ref, right_ref, out_ref):
    r = lax.broadcasted_iota(jnp.int32, (384, 384), 0)
    c = lax.broadcasted_iota(jnp.int32, (384, 384), 1)
    second = r >= 192
    k = jnp.where(second, r - 192, r)
    source = k + 12 * ((k * 171) >> 11) + jnp.where(second, 12, 0)
    sort = jnp.where(c == source, 1.0, 0.0).astype(bf16)
    half_a = jnp.dot(sort, w_ref[0:384, :], preferred_element_type=f32).astype(bf16)
    half_b = jnp.dot(sort, w_ref[384:768, :], preferred_element_type=f32).astype(bf16)
    blocks = [left_ref[0], left_ref[1]] + [own_ref[k] for k in range(4)]
    blocks += [right_ref[0], right_ref[1]]
    parts = []
    for which in range(2):
        rows = jnp.concatenate([b[16 * which : 16 * which + 16] for b in blocks], axis=0)
        part = jnp.dot(
            rows[:, 0:192], half_a[192 * which : 192 * which + 192], preferred_element_type=f32
        ) + jnp.dot(
            rows[:, 192:384], half_b[192 * which : 192 * which + 192], preferred_element_type=f32
        )
        parts.append(part.astype(bf16))
    for y in range(4):
        for m in range(4):
            for place, block in enumerate((y + 2, y + 2 + DELTA[m])):
                for which in range(2):
                    start = 32 * place + 16 * which
                    out_ref[4 * y + m, start : start + 16, :] = parts[which][
                        16 * block : 16 * block + 16
                    ]


def embed(where_ref, got_ref, pair_ref, own_ref, out_ref, rows_ref):
    z = where_ref[1]
    m = where_ref[2]
    pres = []
    total = None
    for col in range(4):
        pre = got_ref[col].astype(f32)
        for part in range(1, 4):
            pre = pre + got_ref[4 * part + col].astype(f32)
        pre = pre.astype(bf16).astype(f32)
        square = jnp.sum(pre * pre, axis=1, keepdims=True)
        total = square if total is None else total + square
        pres.append(pre)
    norm = lax.rsqrt(total + epsilon)
    for col in range(4):
        rows_ref[:, 288 * col : 288 * col + 288] = (pres[col] * norm).astype(bf16)
    for place in range(2):
        high = jnp.broadcast_to(pair_ref[place, 0:1, :], (8, 128))
        low = jnp.broadcast_to(pair_ref[place, 1:2, :], (8, 128))
        tile = jnp.concatenate([high, low], axis=0).astype(bf16)
        rows_ref[32 * place : 32 * place + 16, 1152:1280] = tile
        rows_ref[32 * place + 16 : 32 * place + 32, 1152:1280] = jnp.zeros((16, 128), bf16)
    own_ref[...] = rows_ref[0:32, 0:1152]
    middle = (m == 1) | (m == 2)
    for to in range(8):
        other_img = middle | ((m == 0) & (z >= to)) | ((m == 3) & (z < to))
        other_txt = middle | ((m == 0) & (z > to)) | ((m == 3) & (z <= to))
        at = pl.multiple_of(jnp.where(other_img, 32, 0), 32)
        out_ref[to, 0:16, :] = rows_ref[pl.ds(at, 16), :]
        at = pl.multiple_of(jnp.where(other_txt, 48, 16), 16)
        out_ref[to, 16:32, :] = rows_ref[pl.ds(at, 16), :]


def score(where_ref, scale_ref, bias_ref, pair_ref, own_ref, got_ref, out_ref):
    octet = where_ref[0]
    z = where_ref[1]
    m = where_ref[2]
    scale = jnp.exp(jnp.full((16, 128), scale_ref[0], f32))
    scale_one = scale[:, 0:1]
    offset = bias_ref[0]
    imgs = jnp.concatenate([got_ref[k, 0:16, 0:1152] for k in range(8)], axis=0)
    txts = jnp.concatenate([got_ref[k, 16:32, 0:1152] for k in range(8)], axis=0)
    codes = got_ref[0, 0:16, 1152:1280].astype(f32)
    for k in range(1, 8):
        codes = codes + got_ref[k, 0:16, 1152:1280].astype(f32)
    pair_window = codes[0:1] * 64.0 + codes[8:9]
    lane = lax.broadcasted_iota(jnp.int32, (16, 128), 1)
    row = lax.broadcasted_iota(jnp.int32, (16, 128), 0)
    there = lane >> 4
    behind = jnp.where(there > z, -2, 0)
    ahead = jnp.where(there > z, 0, 2)
    delta = jnp.where(m == 0, behind, jnp.where(m == 3, ahead, jnp.where(m == 1, -1, 1)))
    block = (8 * (octet + delta) + there) & 127
    text_index = block * 16 + (lane & 15)
    match_img = pair_ref[...] == text_index
    own_text = (octet * 8 + z) * 16 + row
    match_txt = pair_window == own_text.astype(f32)

    def grads(own, window, match):
        scores = lax.dot_general(own, window, (((1,), (1,)), ((), ())), preferred_element_type=f32)
        logits = scale * scores + offset
        label = jnp.where(match, 1.0, -1.0)
        coef = (-label / (1.0 + jnp.exp(label * logits))).astype(bf16)
        return scale_one * jnp.dot(coef, window, preferred_element_type=f32)

    image_part = grads(own_ref[0:16, :], txts, match_img)
    text_part = grads(own_ref[16:32, :], imgs, match_txt)
    for to in range(4):
        out_ref[to, 0:16, :] = image_part[:, 288 * to : 288 * to + 288].astype(out_ref.dtype)
        rows = text_part[4 * to : 4 * to + 4]
        out_ref[to, 16:32, :] = jnp.concatenate(
            [rows[:, 288 * c : 288 * c + 288] for c in range(4)], axis=0
        ).astype(out_ref.dtype)


def finish(got_ref, image_ref, text_ref):
    total = got_ref[0].astype(f32)
    for k in range(1, 4):
        total = total + got_ref[k].astype(f32)
    image_ref[...] = total[0:16]
    for c in range(4):
        text_ref[:, 288 * c : 288 * c + 288] = total[16 + 4 * c : 20 + 4 * c]


def exchange(value, axes):
    return lax.all_to_all(value, axes, split_axis=0, concat_axis=0, tiled=True)


def local(img_feat, txt_feat, w_img, w_txt, pair_index, log_scale, bias):
    x, y, z = (lax.axis_index(a) for a in BATCH)
    m = lax.axis_index(MP)
    octet = 4 * x + y
    where = jnp.stack([octet, z, m]).astype(jnp.int32)

    lane = jnp.arange(384, dtype=jnp.int32)
    spread = jnp.tile(pair_index, 24)
    here = (lane // 16) == z
    codes = jnp.stack([jnp.where(here, spread // 64, 0), jnp.where(here, spread % 64, 0)])
    codes = jnp.concatenate([codes.astype(bf16), jnp.zeros((6, 384), bf16)], axis=0)
    feats = jnp.concatenate([img_feat, txt_feat], axis=0).reshape(32, 4, 4, 96)
    feats = feats.transpose(2, 0, 1, 3).reshape(4, 32, 384)
    sent = jnp.concatenate([feats, jnp.broadcast_to(codes, (4, 8, 384))], axis=1)
    own = exchange(sent, "y")
    up = [(s, (s + 1) % 4) for s in range(4)]
    down = [(s, (s - 1) % 4) for s in range(4)]
    left = lax.ppermute(own[2:4], "x", up)
    right = lax.ppermute(own[0:2], "x", down)

    weights = jnp.concatenate([w_img, w_txt], axis=0)
    weights = exchange(jnp.broadcast_to(weights, (32, 24, 288)), ("x", "z"))
    weights = weights.reshape(768, 288)

    sent = call(
        project, jax.ShapeDtypeStruct((16, 64, 288), bf16), [], weights, left, own, right
    )
    got = exchange(sent, ("y",) + MP)

    codes = jnp.concatenate([a[:, 32:34, 0:128] for a in (left, own, right)], axis=0)
    codes = codes.astype(f32)
    delta = jnp.where(m < 2, m - 2, m - 1)
    pairs = jnp.concatenate(
        [
            lax.dynamic_slice_in_dim(codes, y + 2, 1, 0),
            lax.dynamic_slice_in_dim(codes, y + 2 + delta, 1, 0),
        ],
        axis=0,
    )
    mine, sent = call(
        embed,
        (jax.ShapeDtypeStruct((32, 1152), bf16), jax.ShapeDtypeStruct((8, 32, 1280), bf16)),
        [pltpu.VMEM((64, 1280), bf16)],
        where,
        got,
        pairs,
        smem=(0,),
    )
    got = exchange(sent, "z")
    sent = call(
        score,
        jax.ShapeDtypeStruct((4, 32, 288), f32),
        [],
        where,
        log_scale,
        bias,
        pair_index.reshape(16, 1),
        mine,
        got,
        smem=(0, 1, 2),
    )
    got = exchange(sent, MP)
    return call(
        finish,
        (jax.ShapeDtypeStruct((16, 288), f32), jax.ShapeDtypeStruct((4, 1152), f32)),
        [],
        got,
    )


def solution(mesh):
    finer = Mesh(mesh.devices.reshape(4, 4, 8, 2, 2), BATCH + MP)
    in_specs = (P(BATCH, None), P(BATCH, None), P(BATCH, MP), P(BATCH, MP), P(BATCH), P(), P())
    out_specs = (P(BATCH, MP), P(BATCH + MP, None))
    return jax.shard_map(local, mesh=finer, in_specs=in_specs, out_specs=out_specs, check_vma=False)
```

```python
import jax
import jax.numpy as jnp
from jax import lax
from jax.experimental import pallas as pl
from jax.experimental.pallas import tpu as pltpu
from jax.sharding import Mesh
from jax.sharding import PartitionSpec as P

BATCH = ("x", "y", "z")
MP = ("m0", "m1")
bf16 = jnp.bfloat16
f32 = jnp.float32
epsilon = 1e-06
DELTA = (-2, -1, 1, 2)


def call(body, out_shape, scratch, *args, smem=()):
    specs = [
        pl.BlockSpec(memory_space=pltpu.SMEM if k in smem else pltpu.VMEM)
        for k in range(len(args))
    ]
    outs = jax.tree.map(lambda _: pl.BlockSpec(memory_space=pltpu.VMEM), out_shape)
    return pl.pallas_call(
        body, out_shape=out_shape, in_specs=specs, out_specs=outs, scratch_shapes=scratch,
        compiler_params=pltpu.CompilerParams(vmem_limit_bytes=16 << 20),
    )(*args)


def project(w_ref, left_ref, own_ref, right_ref, out_ref):
    r = lax.broadcasted_iota(jnp.int32, (384, 384), 0)
    c = lax.broadcasted_iota(jnp.int32, (384, 384), 1)
    second = r >= 192
    k = jnp.where(second, r - 192, r)
    source = k + 12 * ((k * 171) >> 11) + jnp.where(second, 12, 0)
    sort = jnp.where(c == source, 1.0, 0.0).astype(bf16)
    half_a = jnp.dot(sort, w_ref[0:384, :], preferred_element_type=f32).astype(bf16)
    half_b = jnp.dot(sort, w_ref[384:768, :], preferred_element_type=f32).astype(bf16)
    blocks = [left_ref[0], left_ref[1]] + [own_ref[k] for k in range(4)]
    blocks += [right_ref[0], right_ref[1]]
    parts = []
    for which in range(2):
        rows = jnp.concatenate([b[16 * which : 16 * which + 16] for b in blocks], axis=0)
        part = jnp.dot(
            rows[:, 0:192], half_a[192 * which : 192 * which + 192], preferred_element_type=f32
        ) + jnp.dot(
            rows[:, 192:384], half_b[192 * which : 192 * which + 192], preferred_element_type=f32
        )
        parts.append(part.astype(bf16))
    for y in range(4):
        for m in range(4):
            for place, block in enumerate((y + 2, y + 2 + DELTA[m])):
                for which in range(2):
                    start = 32 * place + 16 * which
                    out_ref[4 * y + m, start : start + 16, :] = parts[which][
                        16 * block : 16 * block + 16
                    ]


def embed(where_ref, got_ref, pair_ref, own_ref, out_ref, rows_ref):
    z = where_ref[1]
    m = where_ref[2]
    pres = []
    total = None
    for col in range(4):
        pre = got_ref[col].astype(f32)
        for part in range(1, 4):
            pre = pre + got_ref[4 * part + col].astype(f32)
        square = jnp.sum(pre * pre, axis=1, keepdims=True)
        total = square if total is None else total + square
        pres.append(pre)
    norm = lax.rsqrt(total + epsilon)
    for col in range(4):
        rows_ref[:, 288 * col : 288 * col + 288] = (pres[col] * norm).astype(bf16)
    for place in range(2):
        high = jnp.broadcast_to(pair_ref[place, 0:1, :], (8, 128))
        low = jnp.broadcast_to(pair_ref[place, 1:2, :], (8, 128))
        tile = jnp.concatenate([high, low], axis=0).astype(bf16)
        rows_ref[32 * place : 32 * place + 16, 1152:1280] = tile
        rows_ref[32 * place + 16 : 32 * place + 32, 1152:1280] = jnp.zeros((16, 128), bf16)
    own_ref[...] = rows_ref[0:32, 0:1152]
    middle = (m == 1) | (m == 2)
    for to in range(8):
        other_img = middle | ((m == 0) & (z >= to)) | ((m == 3) & (z < to))
        other_txt = middle | ((m == 0) & (z > to)) | ((m == 3) & (z <= to))
        at = pl.multiple_of(jnp.where(other_img, 32, 0), 32)
        out_ref[to, 0:16, :] = rows_ref[pl.ds(at, 16), :]
        at = pl.multiple_of(jnp.where(other_txt, 48, 16), 16)
        out_ref[to, 16:32, :] = rows_ref[pl.ds(at, 16), :]


def score(where_ref, scale_ref, bias_ref, pair_ref, own_ref, got_ref, out_ref):
    octet = where_ref[0]
    z = where_ref[1]
    m = where_ref[2]
    scale = jnp.exp(jnp.full((16, 128), scale_ref[0], f32))
    scale_one = scale[:, 0:1]
    offset = bias_ref[0]
    imgs = jnp.concatenate([got_ref[k, 0:16, 0:1152] for k in range(8)], axis=0)
    txts = jnp.concatenate([got_ref[k, 16:32, 0:1152] for k in range(8)], axis=0)
    codes = got_ref[0, 0:16, 1152:1280].astype(f32)
    for k in range(1, 8):
        codes = codes + got_ref[k, 0:16, 1152:1280].astype(f32)
    pair_window = codes[0:1] * 64.0 + codes[8:9]
    lane = lax.broadcasted_iota(jnp.int32, (16, 128), 1)
    row = lax.broadcasted_iota(jnp.int32, (16, 128), 0)
    there = lane >> 4
    behind = jnp.where(there > z, -2, 0)
    ahead = jnp.where(there > z, 0, 2)
    delta = jnp.where(m == 0, behind, jnp.where(m == 3, ahead, jnp.where(m == 1, -1, 1)))
    block = (8 * (octet + delta) + there) & 127
    text_index = block * 16 + (lane & 15)
    match_img = pair_ref[...] == text_index
    own_text = (octet * 8 + z) * 16 + row
    match_txt = pair_window == own_text.astype(f32)

    def grads(own, window, match):
        scores = lax.dot_general(own, window, (((1,), (1,)), ((), ())), preferred_element_type=f32)
        logits = scale * scores + offset
        label = jnp.where(match, 1.0, -1.0)
        coef = (-label / (1.0 + jnp.exp(label * logits))).astype(bf16)
        return scale_one * jnp.dot(coef, window, preferred_element_type=f32)

    image_part = grads(own_ref[0:16, :], txts, match_img)
    text_part = grads(own_ref[16:32, :], imgs, match_txt)
    for to in range(4):
        out_ref[to, 0:16, :] = image_part[:, 288 * to : 288 * to + 288].astype(out_ref.dtype)
        rows = text_part[4 * to : 4 * to + 4]
        out_ref[to, 16:32, :] = jnp.concatenate(
            [rows[:, 288 * c : 288 * c + 288] for c in range(4)], axis=0
        ).astype(out_ref.dtype)


def finish(got_ref, image_ref, text_ref):
    total = got_ref[0].astype(f32)
    for k in range(1, 4):
        total = total + got_ref[k].astype(f32)
    image_ref[...] = total[0:16]
    for c in range(4):
        text_ref[:, 288 * c : 288 * c + 288] = total[16 + 4 * c : 20 + 4 * c]


def exchange(value, axes):
    return lax.all_to_all(value, axes, split_axis=0, concat_axis=0, tiled=True)


def local(img_feat, txt_feat, w_img, w_txt, pair_index, log_scale, bias):
    x, y, z = (lax.axis_index(a) for a in BATCH)
    m = lax.axis_index(MP)
    octet = 4 * x + y
    where = jnp.stack([octet, z, m]).astype(jnp.int32)

    lane = jnp.arange(384, dtype=jnp.int32)
    spread = jnp.tile(pair_index, 24)
    here = (lane // 16) == z
    codes = jnp.stack([jnp.where(here, spread // 64, 0), jnp.where(here, spread % 64, 0)])
    codes = jnp.concatenate([codes.astype(bf16), jnp.zeros((6, 384), bf16)], axis=0)
    feats = jnp.concatenate([img_feat, txt_feat], axis=0).reshape(32, 4, 4, 96)
    feats = feats.transpose(2, 0, 1, 3).reshape(4, 32, 384)
    sent = jnp.concatenate([feats, jnp.broadcast_to(codes, (4, 8, 384))], axis=1)
    own = exchange(sent, "y")
    up = [(s, (s + 1) % 4) for s in range(4)]
    down = [(s, (s - 1) % 4) for s in range(4)]
    left = lax.ppermute(own[2:4], "x", up)
    right = lax.ppermute(own[0:2], "x", down)

    weights = jnp.concatenate([w_img, w_txt], axis=0)
    weights = exchange(jnp.broadcast_to(weights, (32, 24, 288)), ("x", "z"))
    weights = weights.reshape(768, 288)

    sent = call(
        project, jax.ShapeDtypeStruct((16, 64, 288), bf16), [], weights, left, own, right
    )
    got = exchange(sent, ("y",) + MP)

    codes = jnp.concatenate([a[:, 32:34, 0:128] for a in (left, own, right)], axis=0)
    codes = codes.astype(f32)
    delta = jnp.where(m < 2, m - 2, m - 1)
    pairs = jnp.concatenate(
        [
            lax.dynamic_slice_in_dim(codes, y + 2, 1, 0),
            lax.dynamic_slice_in_dim(codes, y + 2 + delta, 1, 0),
        ],
        axis=0,
    )
    mine, sent = call(
        embed,
        (jax.ShapeDtypeStruct((32, 1152), bf16), jax.ShapeDtypeStruct((8, 32, 1280), bf16)),
        [pltpu.VMEM((64, 1280), bf16)],
        where,
        got,
        pairs,
        smem=(0,),
    )
    got = exchange(sent, "z")
    sent = call(
        score,
        jax.ShapeDtypeStruct((4, 32, 288), bf16),
        [],
        where,
        log_scale,
        bias,
        pair_index.reshape(16, 1),
        mine,
        got,
        smem=(0, 1, 2),
    )
    got = exchange(sent, MP)
    return call(
        finish,
        (jax.ShapeDtypeStruct((16, 288), f32), jax.ShapeDtypeStruct((4, 1152), f32)),
        [],
        got,
    )


def solution(mesh):
    finer = Mesh(mesh.devices.reshape(4, 4, 8, 2, 2), BATCH + MP)
    in_specs = (P(BATCH, None), P(BATCH, None), P(BATCH, MP), P(BATCH, MP), P(BATCH), P(), P())
    out_specs = (P(BATCH, MP), P(BATCH + MP, None))
    return jax.shard_map(local, mesh=finer, in_specs=in_specs, out_specs=out_specs, check_vma=False)
```

```python
import jax
import jax.numpy as jnp
from jax import lax
from jax.experimental import pallas as pl
from jax.experimental.pallas import tpu as pltpu
from jax.sharding import Mesh
from jax.sharding import PartitionSpec as P


BATCH = ("x", "y", "z")
MP = ("m0", "m1")
bf16 = jnp.bfloat16
f32 = jnp.float32
epsilon = 1e-06
DELTA = (-2, -1, 1, 2)


def call(body, out_shape, scratch, *args, smem=()):
    specs = [
        pl.BlockSpec(memory_space=pltpu.SMEM if k in smem else pltpu.VMEM)
        for k in range(len(args))
    ]
    outs = jax.tree.map(lambda _: pl.BlockSpec(memory_space=pltpu.VMEM), out_shape)
    return pl.pallas_call(
        body, out_shape=out_shape, in_specs=specs, out_specs=outs, scratch_shapes=scratch,
        compiler_params=pltpu.CompilerParams(vmem_limit_bytes=16 << 20),
    )(*args)


def pack(img_ref, txt_ref, out_ref):
    both = jnp.concatenate([img_ref[...].astype(f32), txt_ref[...].astype(f32)], axis=0)
    tail = jnp.concatenate([both[6 * g : 6 * g + 6, 256:288] for g in range(4)], axis=1)
    rows = [both[:, 0:128], both[:, 128:256], tail, jnp.zeros((2, 128), f32)]
    rows = jnp.concatenate(rows, axis=0).astype(bf16)
    for k in range(out_ref.shape[0]):
        out_ref[k] = rows


def project(where_ref, w_ref, r0_ref, r1_ref, r2_ref, r3_ref, out_ref, codes_ref, feat_ref):
    r = lax.broadcasted_iota(jnp.int32, (384, 384), 0)
    c = lax.broadcasted_iota(jnp.int32, (384, 384), 1)
    second = r >= 192
    k = jnp.where(second, r - 192, r)
    source = k + 12 * ((k * 171) >> 11) + jnp.where(second, 12, 0)
    sort = jnp.where(c == source, 1.0, 0.0).astype(bf16)
    k = lax.broadcasted_iota(jnp.int32, (192, 128), 0)
    c = lax.broadcasted_iota(jnp.int32, (192, 128), 1)
    group = (k * 171) >> 11
    inner = k - 12 * group
    low = jnp.where((inner < 6) & (c == 8 * group + inner), 1.0, 0.0).astype(bf16)
    high = jnp.where((inner >= 6) & (c == 8 * group + inner - 6), 1.0, 0.0).astype(bf16)
    weights = [[], []]
    for half in range(2):
        some = w_ref[16 * half : 16 * half + 16]
        main = jnp.concatenate(
            [some[:, 0:24].reshape(384, 128), some[:, 24:48].reshape(384, 128)], axis=1
        )
        tail = some[:, 48:56].reshape(128, 128)
        main = jnp.dot(sort, main, preferred_element_type=f32).astype(bf16)
        low_tail = jnp.dot(low, tail, preferred_element_type=f32)
        high_tail = jnp.dot(high, tail, preferred_element_type=f32)
        for which in range(2):
            at = 64 * which
            tail = low_tail[:, at : at + 32] + high_tail[:, at + 32 : at + 64]
            tail = tail.astype(bf16)
            weights[which].append(
                jnp.concatenate([main[192 * which : 192 * which + 192]] + [tail] * 4, axis=1)
            )
    y = where_ref[3]
    for k, ref in enumerate((r0_ref, r1_ref, r2_ref, r3_ref)):
        feat_ref[(y - k) & 3] = ref[...]
    blocks = [(2, 1), (3, 1), (0, 0), (1, 0), (2, 0), (3, 0), (0, 1), (1, 1)]
    for j, (source, kind) in enumerate(blocks):
        codes_ref[j] = feat_ref[source, kind, 32:40, 0:128].astype(f32)
    parts = []
    for which in range(2):
        rows = jnp.concatenate(
            [feat_ref[s, kind, 16 * which : 16 * which + 16, :] for s, kind in blocks], axis=0
        )
        part = jnp.dot(rows[:, 0:192], weights[which][0], preferred_element_type=f32)
        part = part + jnp.dot(rows[:, 192:384], weights[which][1], preferred_element_type=f32)
        parts.append(part.astype(bf16))
    for y in range(4):
        for m in range(4):
            for place, block in enumerate((y + 2, y + 2 + DELTA[m])):
                for which in range(2):
                    piece = 2 * place + which
                    rows = parts[which][16 * block : 16 * block + 16]
                    to = 4 * y + m
                    at = 16 * piece
                    out_ref[to, at : at + 16, :] = rows[:, 0:128]
                    out_ref[to, 64 + at : 80 + at, :] = rows[:, 128:256]
                    out_ref[to, 128:144, 32 * piece : 32 * piece + 32] = rows[
                        :, 256 + 32 * piece : 288 + 32 * piece
                    ]


def embed(where_ref, got_ref, pair_ref, own_ref, out_ref, rows_ref):
    z = where_ref[1]
    m = where_ref[2]
    total = jnp.zeros((64, 1), f32)
    mains = []
    tails = []
    for col in range(4):
        pre = got_ref[col].astype(f32)
        for part in range(1, 4):
            pre = pre + got_ref[4 * part + col].astype(f32)
        mains += [pre[0:64], pre[64:128]]
        last = pre[128:144]
        tails.append(
            jnp.concatenate([last[:, 32 * g : 32 * g + 32] for g in range(4)], axis=0)
        )
    mains.append(jnp.concatenate(tails, axis=1))
    for pre in mains:
        total = total + jnp.sum(pre * pre, axis=1, keepdims=True)
    norm = lax.rsqrt(total + epsilon)
    for tile, pre in enumerate(mains):
        rows_ref[:, 128 * tile : 128 * tile + 128] = (pre * norm).astype(bf16)
    other = where_ref[3] + 2 + jnp.where(m < 2, m - 2, m - 1)
    for place in range(2):
        at = where_ref[3] + 2 if place == 0 else other
        code = pair_ref[at]
        high = jnp.broadcast_to(code[0:1, :], (8, 128))
        low = jnp.broadcast_to(code[1:2, :], (8, 128))
        tile = jnp.concatenate([high, low], axis=0).astype(bf16)
        rows_ref[32 * place : 32 * place + 16, 1152:1280] = tile
        rows_ref[32 * place + 16 : 32 * place + 32, 1152:1280] = jnp.zeros((16, 128), bf16)
    own_ref[...] = rows_ref[0:32, 0:1152]
    middle = (m == 1) | (m == 2)
    for to in range(8):
        other_img = middle | ((m == 0) & (z >= to)) | ((m == 3) & (z < to))
        other_txt = middle | ((m == 0) & (z > to)) | ((m == 3) & (z <= to))
        at = pl.multiple_of(jnp.where(other_img, 32, 0), 32)
        out_ref[to, 0:16, :] = rows_ref[pl.ds(at, 16), :]
        at = pl.multiple_of(jnp.where(other_txt, 48, 16), 16)
        out_ref[to, 16:32, :] = rows_ref[pl.ds(at, 16), :]


def score(where_ref, scale_ref, bias_ref, pair_ref, own_ref, got_ref, out_ref):
    octet = where_ref[0]
    z = where_ref[1]
    m = where_ref[2]
    scale = jnp.exp(jnp.full((16, 128), scale_ref[0], f32))
    scale_one = scale[:, 0:1]
    offset = bias_ref[0]
    imgs = jnp.concatenate([got_ref[k, 0:16, 0:1152] for k in range(8)], axis=0)
    txts = jnp.concatenate([got_ref[k, 16:32, 0:1152] for k in range(8)], axis=0)
    codes = got_ref[0, 0:16, 1152:1280].astype(f32)
    for k in range(1, 8):
        codes = codes + got_ref[k, 0:16, 1152:1280].astype(f32)
    pair_window = codes[0:1] * 64.0 + codes[8:9]
    lane = lax.broadcasted_iota(jnp.int32, (16, 128), 1)
    row = lax.broadcasted_iota(jnp.int32, (16, 128), 0)
    there = lane >> 4
    behind = jnp.where(there > z, -2, 0)
    ahead = jnp.where(there > z, 0, 2)
    delta = jnp.where(m == 0, behind, jnp.where(m == 3, ahead, jnp.where(m == 1, -1, 1)))
    block = (8 * (octet + delta) + there) & 127
    text_index = block * 16 + (lane & 15)
    match_img = pair_ref[...] == text_index
    own_text = (octet * 8 + z) * 16 + row
    match_txt = pair_window == own_text.astype(f32)

    def grads(own, window, match):
        scores = lax.dot_general(own, window, (((1,), (1,)), ((), ())), preferred_element_type=f32)
        logits = scale * scores + offset
        label = jnp.where(match, 1.0, -1.0)
        coef = (-label / (1.0 + jnp.exp(label * logits))).astype(bf16)
        return scale_one * jnp.dot(coef, window, preferred_element_type=f32)

    image_part = grads(own_ref[0:16, :], txts, match_img)
    text_part = grads(own_ref[16:32, :], imgs, match_txt)
    for to in range(4):
        out_ref[to, 0:16, :] = jnp.concatenate(
            [
                image_part[:, 256 * to : 256 * to + 256],
                image_part[:, 1024 + 32 * to : 1056 + 32 * to],
            ],
            axis=1,
        ).astype(out_ref.dtype)
        rows = text_part[4 * to : 4 * to + 4]
        out_ref[to, 16:32, :] = jnp.concatenate(
            [
                jnp.concatenate(
                    [rows[:, 256 * c : 256 * c + 256], rows[:, 1024 + 32 * c : 1056 + 32 * c]],
                    axis=1,
                )
                for c in range(4)
            ],
            axis=0,
        ).astype(out_ref.dtype)


def finish(got_ref, image_ref, text_ref):
    total = got_ref[0].astype(f32)
    for k in range(1, 4):
        total = total + got_ref[k].astype(f32)
    image_ref[...] = total[0:16]
    for c in range(4):
        text_ref[:, 288 * c : 288 * c + 288] = total[16 + 4 * c : 20 + 4 * c]


def exchange(value, axes):
    return lax.all_to_all(value, axes, split_axis=0, concat_axis=0, tiled=True)


def local(img_feat, txt_feat, w_img, w_txt, pair_index, log_scale, bias):
    x, y, z = (lax.axis_index(a) for a in BATCH)
    m = lax.axis_index(MP)
    octet = 4 * x + y
    where = jnp.stack([octet, z, m, y]).astype(jnp.int32)

    sent = call(pack, jax.ShapeDtypeStruct((32, 56, 128), bf16), [], w_img, w_txt)
    weights = exchange(sent, ("x", "z"))

    lane = jnp.arange(384, dtype=jnp.int32)
    spread = jnp.tile(pair_index, 24)
    here = (lane // 16) == z
    codes = jnp.stack([jnp.where(here, spread // 64, 0), jnp.where(here, spread % 64, 0)])
    codes = jnp.concatenate([codes.astype(bf16), jnp.zeros((6, 384), bf16)], axis=0)
    feats = jnp.concatenate([img_feat, txt_feat], axis=0).reshape(32, 4, 4, 96)
    feats = feats.transpose(2, 0, 1, 3).reshape(4, 32, 384)
    feats = jnp.concatenate([feats, jnp.broadcast_to(codes, (4, 8, 384))], axis=1)
    pairs = []
    for s in range(16):
        up, slot = divmod(s, 4)
        pairs.append((s, 4 * ((up + (1 if slot > 1 else -1)) % 4) + slot))
    far = lax.ppermute(feats, ("x", "y"), pairs)
    both = jnp.stack([feats, far], axis=1)
    received = [lax.dynamic_index_in_dim(both, y, 0, keepdims=False)]
    for k in range(1, 4):
        chosen = lax.dynamic_index_in_dim(both, (y + k) % 4, 0, keepdims=False)
        received.append(
            lax.ppermute(chosen, "y", [(s, (s + k) % 4) for s in range(4)])
        )

    sent, codes = call(
        project,
        (jax.ShapeDtypeStruct((16, 144, 128), bf16), jax.ShapeDtypeStruct((8, 8, 128), f32)),
        [pltpu.VMEM((4, 2, 40, 384), bf16)],
        where,
        weights,
        *received,
        smem=(0,),
    )
    got = exchange(sent, ("y",) + MP)
    mine, sent = call(
        embed,
        (jax.ShapeDtypeStruct((32, 1152), bf16), jax.ShapeDtypeStruct((8, 32, 1280), bf16)),
        [pltpu.VMEM((64, 1280), bf16)],
        where,
        got,
        codes,
        smem=(0,),
    )
    got = exchange(sent, "z")
    sent = call(
        score,
        jax.ShapeDtypeStruct((4, 32, 288), bf16),
        [],
        where,
        log_scale,
        bias,
        pair_index.reshape(16, 1),
        mine,
        got,
        smem=(0, 1, 2),
    )
    got = exchange(sent, MP)
    return call(
        finish,
        (jax.ShapeDtypeStruct((16, 288), f32), jax.ShapeDtypeStruct((4, 1152), f32)),
        [],
        got,
    )


def solution(mesh):
    finer = Mesh(mesh.devices.reshape(4, 4, 8, 2, 2), BATCH + MP)
    in_specs = (P(BATCH, None), P(BATCH, None), P(BATCH, MP), P(BATCH, MP), P(BATCH), P(), P())
    out_specs = (P(BATCH, MP), P(BATCH + MP, None))

    return jax.shard_map(local, mesh=finer, in_specs=in_specs, out_specs=out_specs, check_vma=False)
```

```python
import jax
import jax.numpy as jnp
from jax import lax
from jax.experimental import pallas as pl
from jax.experimental.pallas import tpu as pltpu
from jax.sharding import Mesh
from jax.sharding import PartitionSpec as P


BATCH = ("x", "y", "z")
MP = ("m0", "m1")
bf16 = jnp.bfloat16
f32 = jnp.float32
epsilon = 1e-06
DELTA = (-2, -1, 1, 2)


def call(body, out_shape, scratch, *args, smem=()):
    specs = [
        pl.BlockSpec(memory_space=pltpu.SMEM if k in smem else pltpu.VMEM)
        for k in range(len(args))
    ]
    outs = jax.tree.map(lambda _: pl.BlockSpec(memory_space=pltpu.VMEM), out_shape)
    return pl.pallas_call(
        body, out_shape=out_shape, in_specs=specs, out_specs=outs, scratch_shapes=scratch,
        compiler_params=pltpu.CompilerParams(vmem_limit_bytes=16 << 20),
    )(*args)


def pack(img_ref, txt_ref, out_ref):
    both = jnp.concatenate([img_ref[...].astype(f32), txt_ref[...].astype(f32)], axis=0)
    tail = jnp.concatenate([both[6 * g : 6 * g + 6, 256:288] for g in range(4)], axis=1)
    rows = [both[:, 0:128], both[:, 128:256], tail, jnp.zeros((2, 128), f32)]
    rows = jnp.concatenate(rows, axis=0).astype(bf16)
    for k in range(out_ref.shape[0]):
        out_ref[k] = rows


def project(where_ref, w_ref, r0_ref, r1_ref, r2_ref, r3_ref, out_ref, feat_ref):
    r = lax.broadcasted_iota(jnp.int32, (384, 384), 0)
    c = lax.broadcasted_iota(jnp.int32, (384, 384), 1)
    second = r >= 192
    k = jnp.where(second, r - 192, r)
    source = k + 12 * ((k * 171) >> 11) + jnp.where(second, 12, 0)
    sort = jnp.where(c == source, 1.0, 0.0).astype(bf16)
    k = lax.broadcasted_iota(jnp.int32, (192, 128), 0)
    c = lax.broadcasted_iota(jnp.int32, (192, 128), 1)
    group = (k * 171) >> 11
    inner = k - 12 * group
    low = jnp.where((inner < 6) & (c == 8 * group + inner), 1.0, 0.0).astype(bf16)
    high = jnp.where((inner >= 6) & (c == 8 * group + inner - 6), 1.0, 0.0).astype(bf16)
    weights = [[], []]
    for half in range(2):
        some = w_ref[16 * half : 16 * half + 16]
        main = jnp.concatenate(
            [some[:, 0:24].reshape(384, 128), some[:, 24:48].reshape(384, 128)], axis=1
        )
        tail = some[:, 48:56].reshape(128, 128)
        main = jnp.dot(sort, main, preferred_element_type=f32).astype(bf16)
        low_tail = jnp.dot(low, tail, preferred_element_type=f32)
        high_tail = jnp.dot(high, tail, preferred_element_type=f32)
        for which in range(2):
            at = 64 * which
            tail = low_tail[:, at : at + 32] + high_tail[:, at + 32 : at + 64]
            tail = tail.astype(bf16)
            weights[which].append(
                jnp.concatenate([main[192 * which : 192 * which + 192]] + [tail] * 4, axis=1)
            )
    y = where_ref[3]
    for k, ref in enumerate((r0_ref, r1_ref, r2_ref, r3_ref)):
        feat_ref[(y - k) & 3] = ref[...]
    parts = []
    for which in range(2):
        rows = jnp.concatenate(
            [feat_ref[s, 16 * which : 16 * which + 16, :] for s in range(4)], axis=0
        )
        part = jnp.dot(rows[:, 0:192], weights[which][0], preferred_element_type=f32)
        parts.append(
            part + jnp.dot(rows[:, 192:384], weights[which][1], preferred_element_type=f32)
        )
    for y in range(4):
        rows = jnp.concatenate([part[16 * y : 16 * y + 16] for part in parts], axis=0)
        tail = jnp.concatenate(
            [rows[8 * g : 8 * g + 8, 256 + 32 * g : 288 + 32 * g] for g in range(4)], axis=1
        )
        block = jnp.concatenate([rows[:, 0:128], rows[:, 128:256], tail], axis=0).astype(bf16)
        for m in range(4):
            out_ref[4 * y + m] = block


def embed(got_ref, codes_ref, own_ref):
    total = jnp.zeros((32, 1), f32)
    tiles = []
    tails = []
    for col in range(4):
        pre = got_ref[col].astype(f32)
        for part in range(1, 4):
            pre = pre + got_ref[4 * part + col].astype(f32)
        tiles += [pre[0:32], pre[32:64]]
        last = pre[64:72]
        tails.append(
            jnp.concatenate([last[:, 32 * g : 32 * g + 32] for g in range(4)], axis=0)
        )
    tiles.append(jnp.concatenate(tails, axis=1))
    for pre in tiles:
        total = total + jnp.sum(pre * pre, axis=1, keepdims=True)
    norm = lax.rsqrt(total + epsilon)
    for t, pre in enumerate(tiles):
        own_ref[32 * t : 32 * t + 32, :] = (pre * norm).astype(bf16)
    own_ref[288:296, :] = codes_ref[...].astype(bf16)


def choose(where_ref, own_ref, other_ref, out_ref, two_ref):
    z = where_ref[1]
    m = where_ref[2]
    two_ref[0] = own_ref[...]
    two_ref[1] = other_ref[...]
    middle = (m == 1) | (m == 2)
    for to in range(8):
        other_img = middle | ((m == 0) & (z >= to)) | ((m == 3) & (z < to))
        other_txt = middle | ((m == 0) & (z > to)) | ((m == 3) & (z <= to))
        img = jnp.where(other_img, 1, 0)
        txt = jnp.where(other_txt, 1, 0)
        for t in range(9):
            out_ref[to, 32 * t : 32 * t + 16, :] = two_ref[img, 32 * t : 32 * t + 16, :]
            out_ref[to, 32 * t + 16 : 32 * t + 32, :] = two_ref[
                txt, 32 * t + 16 : 32 * t + 32, :
            ]
        out_ref[to, 288:296, :] = two_ref[img, 288:296, :]


def score(where_ref, scale_ref, bias_ref, pair_ref, own_ref, got_ref, out_ref):
    octet = where_ref[0]
    z = where_ref[1]
    m = where_ref[2]
    scale = jnp.exp(jnp.full((16, 128), scale_ref[0], f32))
    scale_one = scale[:, 0:1]
    offset = bias_ref[0]

    def window(at):
        return jnp.concatenate(
            [
                jnp.concatenate(
                    [got_ref[k, 32 * t + at : 32 * t + at + 16, :] for k in range(8)], axis=0
                )
                for t in range(9)
            ],
            axis=1,
        )

    def mine(at):
        return jnp.concatenate(
            [own_ref[32 * t + at : 32 * t + at + 16, :] for t in range(9)], axis=1
        )

    imgs = window(0)
    txts = window(16)
    codes = got_ref[0, 288:296, :].astype(f32)
    for k in range(1, 8):
        codes = codes + got_ref[k, 288:296, :].astype(f32)
    pair_window = codes[0:1] * 64.0 + codes[1:2]
    lane = lax.broadcasted_iota(jnp.int32, (16, 128), 1)
    row = lax.broadcasted_iota(jnp.int32, (16, 128), 0)
    there = lane >> 4
    behind = jnp.where(there > z, -2, 0)
    ahead = jnp.where(there > z, 0, 2)
    delta = jnp.where(m == 0, behind, jnp.where(m == 3, ahead, jnp.where(m == 1, -1, 1)))
    block = (8 * (octet + delta) + there) & 127
    text_index = block * 16 + (lane & 15)
    match_img = pair_ref[...] == text_index
    own_text = (octet * 8 + z) * 16 + row
    match_txt = pair_window == own_text.astype(f32)

    def grads(own, window, match):
        scores = lax.dot_general(own, window, (((1,), (1,)), ((), ())), preferred_element_type=f32)
        logits = scale * scores + offset
        label = jnp.where(match, 1.0, -1.0)
        coef = (-label / (1.0 + jnp.exp(label * logits))).astype(bf16)
        return scale_one * jnp.dot(coef, window, preferred_element_type=f32)

    image_part = grads(mine(0), txts, match_img)
    text_part = grads(mine(16), imgs, match_txt)
    for to in range(4):
        rows = text_part[4 * to : 4 * to + 4]
        at = 1024 + 32 * to
        pieces = [
            image_part[:, 256 * to : 256 * to + 128],
            image_part[:, 256 * to + 128 : 256 * to + 256],
        ]
        pieces += [rows[:, 128 * t : 128 * t + 128] for t in range(9)]
        pieces.append(
            jnp.concatenate(
                [image_part[4 * g : 4 * g + 4, at : at + 32] for g in range(4)], axis=1
            )
        )
        out_ref[to] = jnp.concatenate(pieces, axis=0).astype(bf16)


def finish(got_ref, image_ref, text_ref):
    total = got_ref[0].astype(f32)
    for k in range(1, 4):
        total = total + got_ref[k].astype(f32)
    image_ref[:, 0:128] = total[0:16]
    image_ref[:, 128:256] = total[16:32]
    image_ref[:, 256:288] = jnp.concatenate(
        [total[68:72, 32 * g : 32 * g + 32] for g in range(4)], axis=0
    )
    pieces = []
    for c in range(4):
        pieces += [total[32 + 8 * c : 36 + 8 * c], total[36 + 8 * c : 40 + 8 * c]]
        pieces.append(total[64:68, 32 * c : 32 * c + 32])
    text_ref[...] = jnp.concatenate(pieces, axis=1)


def exchange(value, axes):
    return lax.all_to_all(value, axes, split_axis=0, concat_axis=0, tiled=True)


def local(img_feat, txt_feat, w_img, w_txt, pair_index, log_scale, bias):
    x, y, z = (lax.axis_index(a) for a in BATCH)
    m = lax.axis_index(MP)
    octet = 4 * x + y
    where = jnp.stack([octet, z, m, y]).astype(jnp.int32)

    sent = call(pack, jax.ShapeDtypeStruct((32, 56, 128), bf16), [], w_img, w_txt)
    weights = exchange(sent, ("x", "z"))

    feats = jnp.concatenate([img_feat, txt_feat], axis=0).reshape(32, 4, 4, 96)
    feats = feats.transpose(2, 0, 1, 3).reshape(4, 32, 384)
    received = [lax.dynamic_index_in_dim(feats, y, 0, keepdims=False)]
    for k in range(1, 4):
        chosen = lax.dynamic_index_in_dim(feats, (y + k) % 4, 0, keepdims=False)
        received.append(
            lax.ppermute(chosen, "y", [(s, (s + k) % 4) for s in range(4)])
        )

    lane = jnp.arange(128, dtype=jnp.int32)
    spread = jnp.tile(pair_index, 8)
    here = (lane // 16) == z
    codes = jnp.stack([jnp.where(here, spread // 64, 0), jnp.where(here, spread % 64, 0)])
    codes = jnp.concatenate([codes.astype(f32), jnp.zeros((6, 128), f32)], axis=0)

    sent = call(
        project,
        jax.ShapeDtypeStruct((16, 72, 128), bf16),
        [pltpu.VMEM((4, 32, 384), bf16)],
        where,
        weights,
        *received,
        smem=(0,),
    )
    got = exchange(sent, ("y",) + MP)
    own = call(embed, jax.ShapeDtypeStruct((296, 128), bf16), [], got, codes)

    pairs = []
    for s in range(512):
        o, rest = divmod(s, 32)
        pairs.append((s, 32 * ((o - DELTA[rest % 4]) % 16) + rest))
    other = lax.ppermute(own, BATCH + MP, pairs)
    sent = call(
        choose,
        jax.ShapeDtypeStruct((8, 296, 128), bf16),
        [pltpu.VMEM((2, 296, 128), bf16)],
        where,
        own,
        other,
        smem=(0,),
    )
    got = exchange(sent, "z")
    sent = call(
        score,
        jax.ShapeDtypeStruct((4, 72, 128), bf16),
        [],
        where,
        log_scale,
        bias,
        pair_index.reshape(16, 1),
        own,
        got,
        smem=(0, 1, 2),
    )
    got = exchange(sent, MP)
    return call(
        finish,
        (jax.ShapeDtypeStruct((16, 288), f32), jax.ShapeDtypeStruct((4, 1152), f32)),
        [],
        got,
    )


def solution(mesh):
    finer = Mesh(mesh.devices.reshape(4, 4, 8, 2, 2), BATCH + MP)
    in_specs = (P(BATCH, None), P(BATCH, None), P(BATCH, MP), P(BATCH, MP), P(BATCH), P(), P())
    out_specs = (P(BATCH, MP), P(BATCH + MP, None))

    return jax.shard_map(local, mesh=finer, in_specs=in_specs, out_specs=out_specs, check_vma=False)
```

```python
import jax
import jax.numpy as jnp
from jax import lax
from jax.experimental import pallas as pl
from jax.experimental.pallas import tpu as pltpu
from jax.sharding import Mesh
from jax.sharding import PartitionSpec as P


BATCH = ("x", "y", "z")
MP = ("m0", "m1")
bf16 = jnp.bfloat16
f32 = jnp.float32
epsilon = 1e-06
DELTA = (-2, -1, 1, 2)


def call(body, out_shape, scratch, *args, smem=(), hbm=()):
    spaces = [
        pltpu.SMEM if k in smem else pltpu.HBM if k in hbm else pltpu.VMEM for k in range(len(args))
    ]
    specs = [pl.BlockSpec(memory_space=space) for space in spaces]
    outs = jax.tree.map(lambda _: pl.BlockSpec(memory_space=pltpu.VMEM), out_shape)
    return pl.pallas_call(
        body, out_shape=out_shape, in_specs=specs, out_specs=outs, scratch_shapes=scratch,
        compiler_params=pltpu.CompilerParams(vmem_limit_bytes=16 << 20),
    )(*args)


def pack(img_ref, txt_ref, out_ref, img, txt, sems):
    copies = [
        pltpu.make_async_copy(img_ref, img, sems.at[0]),
        pltpu.make_async_copy(txt_ref, txt, sems.at[1]),
    ]
    for copy in copies:
        copy.start()
    for copy in copies:
        copy.wait()
    both = jnp.concatenate([img[...].astype(f32), txt[...].astype(f32)], axis=0)
    tail = jnp.concatenate([both[6 * g : 6 * g + 6, 256:288] for g in range(4)], axis=1)
    rows = [both[:, 0:128], both[:, 128:256], tail, jnp.zeros((2, 128), f32)]
    rows = jnp.concatenate(rows, axis=0).astype(bf16)
    for k in range(out_ref.shape[0]):
        out_ref[k] = rows


def setup(where_ref, pair_ref, scale_ref, bias_ref, sort_ref, split_ref, pairs_ref, consts_ref):
    r = lax.broadcasted_iota(jnp.int32, (384, 384), 0)
    c = lax.broadcasted_iota(jnp.int32, (384, 384), 1)
    second = r >= 192
    k = jnp.where(second, r - 192, r)
    source = k + 12 * ((k * 171) >> 11) + jnp.where(second, 12, 0)
    sort_ref[...] = jnp.where(c == source, 1.0, 0.0).astype(bf16)
    k = lax.broadcasted_iota(jnp.int32, (192, 128), 0)
    c = lax.broadcasted_iota(jnp.int32, (192, 128), 1)
    group = (k * 171) >> 11
    inner = k - 12 * group
    low = (inner < 6) & (c == 8 * group + inner)
    high = (inner >= 6) & (c == 8 * group + inner - 6)
    split_ref[0:192, :] = jnp.where(low, 1.0, 0.0).astype(bf16)
    split_ref[192:384, :] = jnp.where(high, 1.0, 0.0).astype(bf16)
    row = lax.broadcasted_iota(jnp.int32, (16, 128), 0)
    lane = lax.broadcasted_iota(jnp.int32, (8, 128), 1)
    down = jnp.zeros((16, 128), jnp.int32)
    across = jnp.zeros((8, 128), jnp.int32)
    for k in range(16):
        down = jnp.where(row == k, pair_ref[k], down)
        across = jnp.where(lane == 16 * where_ref[1] + k, pair_ref[k], across)
    pairs_ref[...] = down
    row = lax.broadcasted_iota(jnp.int32, (8, 128), 0)
    consts_ref[0:8, :] = jnp.where(row == 0, across >> 6, across & 63).astype(f32)
    consts_ref[8:16, :] = jnp.full((8, 128), scale_ref[0], f32)
    consts_ref[16:24, :] = jnp.full((8, 128), bias_ref[0], f32)


def project(
    where_ref, sort_ref, split_ref, w_ref, r0_ref, r1_ref, r2_ref, r3_ref, out_ref, feat_ref
):
    sort = sort_ref[...]
    low = split_ref[0:192, :]
    high = split_ref[192:384, :]
    weights = [[], []]
    for half in range(2):
        some = w_ref[16 * half : 16 * half + 16]
        main = jnp.concatenate(
            [some[:, 0:24].reshape(384, 128), some[:, 24:48].reshape(384, 128)], axis=1
        )
        tail = some[:, 48:56].reshape(128, 128)
        main = jnp.dot(sort, main, preferred_element_type=f32).astype(bf16)
        low_tail = jnp.dot(low, tail, preferred_element_type=f32)
        high_tail = jnp.dot(high, tail, preferred_element_type=f32)
        for which in range(2):
            at = 64 * which
            tail = low_tail[:, at : at + 32] + high_tail[:, at + 32 : at + 64]
            tail = tail.astype(bf16)
            weights[which].append(
                jnp.concatenate([main[192 * which : 192 * which + 192]] + [tail] * 4, axis=1)
            )
    y = where_ref[3]
    for k, ref in enumerate((r0_ref, r1_ref, r2_ref, r3_ref)):
        feat_ref[(y - k) & 3] = ref[...]
    parts = []
    for which in range(2):
        rows = jnp.concatenate(
            [feat_ref[s, 16 * which : 16 * which + 16, :] for s in range(4)], axis=0
        )
        part = jnp.dot(rows[:, 0:192], weights[which][0], preferred_element_type=f32)
        parts.append(
            part + jnp.dot(rows[:, 192:384], weights[which][1], preferred_element_type=f32)
        )
    for y in range(4):
        rows = jnp.concatenate([part[16 * y : 16 * y + 16] for part in parts], axis=0)
        tail = jnp.concatenate(
            [rows[8 * g : 8 * g + 8, 256 + 32 * g : 288 + 32 * g] for g in range(4)], axis=1
        )
        block = jnp.concatenate([rows[:, 0:128], rows[:, 128:256], tail], axis=0).astype(bf16)
        for m in range(4):
            out_ref[4 * y + m] = block


def embed(got_ref, consts_ref, own_ref):
    total = jnp.zeros((32, 1), f32)
    tiles = []
    tails = []
    for col in range(4):
        pre = got_ref[col].astype(f32)
        for part in range(1, 4):
            pre = pre + got_ref[4 * part + col].astype(f32)
        tiles += [pre[0:32], pre[32:64]]
        last = pre[64:72]
        tails.append(
            jnp.concatenate([last[:, 32 * g : 32 * g + 32] for g in range(4)], axis=0)
        )
    tiles.append(jnp.concatenate(tails, axis=1))
    for pre in tiles:
        total = total + jnp.sum(pre * pre, axis=1, keepdims=True)
    norm = lax.rsqrt(total + epsilon)
    for t, pre in enumerate(tiles):
        own_ref[32 * t : 32 * t + 32, :] = (pre * norm).astype(bf16)
    own_ref[288:296, :] = consts_ref[0:8, :].astype(bf16)


def choose(where_ref, own_ref, other_ref, out_ref, two_ref):
    z = where_ref[1]
    m = where_ref[2]
    two_ref[0] = own_ref[...]
    two_ref[1] = other_ref[...]
    middle = (m == 1) | (m == 2)
    for to in range(8):
        other_img = middle | ((m == 0) & (z >= to)) | ((m == 3) & (z < to))
        other_txt = middle | ((m == 0) & (z > to)) | ((m == 3) & (z <= to))
        img = jnp.where(other_img, 1, 0)
        txt = jnp.where(other_txt, 1, 0)
        for t in range(9):
            out_ref[to, 32 * t : 32 * t + 16, :] = two_ref[img, 32 * t : 32 * t + 16, :]
            out_ref[to, 32 * t + 16 : 32 * t + 32, :] = two_ref[
                txt, 32 * t + 16 : 32 * t + 32, :
            ]
        out_ref[to, 288:296, :] = two_ref[img, 288:296, :]


def score(where_ref, consts_ref, pair_ref, own_ref, got_ref, out_ref):
    octet = where_ref[0]
    z = where_ref[1]
    m = where_ref[2]
    scale = jnp.exp(consts_ref[8:9, :])
    scale_one = scale[:, 0:1]
    offset = consts_ref[16:17, :]

    def window(at):
        return jnp.concatenate(
            [
                jnp.concatenate(
                    [got_ref[k, 32 * t + at : 32 * t + at + 16, :] for k in range(8)], axis=0
                )
                for t in range(9)
            ],
            axis=1,
        )

    def mine(at):
        return jnp.concatenate(
            [own_ref[32 * t + at : 32 * t + at + 16, :] for t in range(9)], axis=1
        )

    imgs = window(0)
    txts = window(16)
    codes = got_ref[0, 288:296, :].astype(f32)
    for k in range(1, 8):
        codes = codes + got_ref[k, 288:296, :].astype(f32)
    pair_window = codes[0:1] * 64.0 + codes[1:2]
    lane = lax.broadcasted_iota(jnp.int32, (16, 128), 1)
    row = lax.broadcasted_iota(jnp.int32, (16, 128), 0)
    there = lane >> 4
    behind = jnp.where(there > z, -2, 0)
    ahead = jnp.where(there > z, 0, 2)
    delta = jnp.where(m == 0, behind, jnp.where(m == 3, ahead, jnp.where(m == 1, -1, 1)))
    block = (8 * (octet + delta) + there) & 127
    text_index = block * 16 + (lane & 15)
    match_img = pair_ref[...] == text_index
    own_text = (octet * 8 + z) * 16 + row
    match_txt = pair_window == own_text.astype(f32)

    def grads(own, window, match):
        scores = lax.dot_general(own, window, (((1,), (1,)), ((), ())), preferred_element_type=f32)
        logits = scale * scores + offset
        label = jnp.where(match, 1.0, -1.0)
        coef = (-label / (1.0 + jnp.exp(label * logits))).astype(bf16)
        return scale_one * jnp.dot(coef, window, preferred_element_type=f32)

    image_part = grads(mine(0), txts, match_img)
    text_part = grads(mine(16), imgs, match_txt)
    for to in range(4):
        rows = text_part[4 * to : 4 * to + 4]
        at = 1024 + 32 * to
        pieces = [
            image_part[:, 256 * to : 256 * to + 128],
            image_part[:, 256 * to + 128 : 256 * to + 256],
        ]
        pieces += [rows[:, 128 * t : 128 * t + 128] for t in range(9)]
        pieces.append(
            jnp.concatenate(
                [image_part[4 * g : 4 * g + 4, at : at + 32] for g in range(4)], axis=1
            )
        )
        out_ref[to] = jnp.concatenate(pieces, axis=0).astype(bf16)


def finish(got_ref, image_ref, text_ref):
    total = got_ref[0].astype(f32)
    for k in range(1, 4):
        total = total + got_ref[k].astype(f32)
    image_ref[:, 0:128] = total[0:16]
    image_ref[:, 128:256] = total[16:32]
    image_ref[:, 256:288] = jnp.concatenate(
        [total[68:72, 32 * g : 32 * g + 32] for g in range(4)], axis=0
    )
    pieces = []
    for c in range(4):
        pieces += [total[32 + 8 * c : 36 + 8 * c], total[36 + 8 * c : 40 + 8 * c]]
        pieces.append(total[64:68, 32 * c : 32 * c + 32])
    text_ref[...] = jnp.concatenate(pieces, axis=1)


def exchange(value, axes):
    return lax.all_to_all(value, axes, split_axis=0, concat_axis=0, tiled=True)


def local(img_feat, txt_feat, w_img, w_txt, pair_index, log_scale, bias):
    x, y, z = (lax.axis_index(a) for a in BATCH)
    m = lax.axis_index(MP)
    octet = 4 * x + y
    where = jnp.stack([octet, z, m, y]).astype(jnp.int32)

    sent = call(
        pack,
        jax.ShapeDtypeStruct((32, 56, 128), bf16),
        [pltpu.VMEM((12, 288), bf16), pltpu.VMEM((12, 288), bf16), pltpu.SemaphoreType.DMA((2,))],
        w_img,
        w_txt,
        hbm=(0, 1),
    )
    weights = exchange(sent, ("x", "z"))

    feats = jnp.concatenate([img_feat, txt_feat], axis=0).reshape(32, 4, 4, 96)
    feats = feats.transpose(2, 0, 1, 3).reshape(4, 32, 384)
    received = [lax.dynamic_index_in_dim(feats, y, 0, keepdims=False)]
    for k in range(1, 4):
        chosen = lax.dynamic_index_in_dim(feats, (y + k) % 4, 0, keepdims=False)
        received.append(
            lax.ppermute(chosen, "y", [(s, (s + k) % 4) for s in range(4)])
        )

    sort, split, pairs, consts = call(
        setup,
        (
            jax.ShapeDtypeStruct((384, 384), bf16),
            jax.ShapeDtypeStruct((384, 128), bf16),
            jax.ShapeDtypeStruct((16, 128), jnp.int32),
            jax.ShapeDtypeStruct((24, 128), f32),
        ),
        [],
        where,
        pair_index,
        log_scale,
        bias,
        smem=(0, 1, 2, 3),
    )

    sent = call(
        project,
        jax.ShapeDtypeStruct((16, 72, 128), bf16),
        [pltpu.VMEM((4, 32, 384), bf16)],
        where,
        sort,
        split,
        weights,
        *received,
        smem=(0,),
    )
    got = exchange(sent, ("y",) + MP)
    own = call(embed, jax.ShapeDtypeStruct((296, 128), bf16), [], got, consts)

    moves = []
    for s in range(512):
        o, rest = divmod(s, 32)
        moves.append((s, 32 * ((o - DELTA[rest % 4]) % 16) + rest))
    other = lax.ppermute(own, BATCH + MP, moves)
    sent = call(
        choose,
        jax.ShapeDtypeStruct((8, 296, 128), bf16),
        [pltpu.VMEM((2, 296, 128), bf16)],
        where,
        own,
        other,
        smem=(0,),
    )
    got = exchange(sent, "z")
    sent = call(
        score,
        jax.ShapeDtypeStruct((4, 72, 128), bf16),
        [],
        where,
        consts,
        pairs,
        own,
        got,
        smem=(0,),
    )
    got = exchange(sent, MP)
    return call(
        finish,
        (jax.ShapeDtypeStruct((16, 288), f32), jax.ShapeDtypeStruct((4, 1152), f32)),
        [],
        got,
    )


def solution(mesh):
    finer = Mesh(mesh.devices.reshape(4, 4, 8, 2, 2), BATCH + MP)
    in_specs = (P(BATCH, None), P(BATCH, None), P(BATCH, MP), P(BATCH, MP), P(BATCH), P(), P())
    out_specs = (P(BATCH, MP), P(BATCH + MP, None))

    return jax.shard_map(local, mesh=finer, in_specs=in_specs, out_specs=out_specs, check_vma=False)
```

```python
import jax
import jax.numpy as jnp
from jax import lax
from jax.experimental import pallas as pl
from jax.experimental.pallas import tpu as pltpu
from jax.sharding import Mesh
from jax.sharding import PartitionSpec as P


BATCH = ("x", "y", "z")
MP = ("m0", "m1")
bf16 = jnp.bfloat16
f32 = jnp.float32
epsilon = 1e-06
DELTA = (-2, -1, 1, 2)


def call(body, out_shape, scratch, *args, smem=(), hbm=(), vmem=16):
    spaces = [
        pltpu.SMEM if k in smem else pltpu.HBM if k in hbm else pltpu.VMEM for k in range(len(args))
    ]
    specs = [pl.BlockSpec(memory_space=space) for space in spaces]
    outs = jax.tree.map(lambda _: pl.BlockSpec(memory_space=pltpu.VMEM), out_shape)
    return pl.pallas_call(
        body, out_shape=out_shape, in_specs=specs, out_specs=outs, scratch_shapes=scratch,
        compiler_params=pltpu.CompilerParams(vmem_limit_bytes=vmem << 20),
    )(*args)


def pack(img_ref, txt_ref, out_ref, img, txt, sems):
    copies = [
        pltpu.make_async_copy(img_ref, img, sems.at[0]),
        pltpu.make_async_copy(txt_ref, txt, sems.at[1]),
    ]
    for copy in copies:
        copy.start()
    for copy in copies:
        copy.wait()
    both = jnp.concatenate([img[...].astype(f32), txt[...].astype(f32)], axis=0)
    tail = jnp.concatenate([both[6 * g : 6 * g + 6, 256:288] for g in range(4)], axis=1)
    rows = [both[:, 0:128], both[:, 128:256], tail, jnp.zeros((2, 128), f32)]
    rows = jnp.concatenate(rows, axis=0).astype(bf16)
    for k in range(out_ref.shape[0]):
        out_ref[k] = rows


def setup(where_ref, pair_ref, scale_ref, bias_ref, sort_ref, split_ref, pairs_ref, consts_ref):
    r = lax.broadcasted_iota(jnp.int32, (384, 384), 0)
    c = lax.broadcasted_iota(jnp.int32, (384, 384), 1)
    second = r >= 192
    k = jnp.where(second, r - 192, r)
    source = k + 12 * ((k * 171) >> 11) + jnp.where(second, 12, 0)
    sort_ref[...] = jnp.where(c == source, 1.0, 0.0).astype(bf16)
    k = lax.broadcasted_iota(jnp.int32, (192, 128), 0)
    c = lax.broadcasted_iota(jnp.int32, (192, 128), 1)
    group = (k * 171) >> 11
    inner = k - 12 * group
    low = (inner < 6) & (c == 8 * group + inner)
    high = (inner >= 6) & (c == 8 * group + inner - 6)
    split_ref[0:192, :] = jnp.where(low, 1.0, 0.0).astype(bf16)
    split_ref[192:384, :] = jnp.where(high, 1.0, 0.0).astype(bf16)
    row = lax.broadcasted_iota(jnp.int32, (16, 128), 0)
    lane = lax.broadcasted_iota(jnp.int32, (8, 128), 1)
    down = jnp.zeros((16, 128), jnp.int32)
    across = jnp.zeros((8, 128), jnp.int32)
    for k in range(16):
        down = jnp.where(row == k, pair_ref[k], down)
        across = jnp.where(lane == 16 * where_ref[1] + k, pair_ref[k], across)
    pairs_ref[...] = down
    row = lax.broadcasted_iota(jnp.int32, (8, 128), 0)
    consts_ref[0:8, :] = jnp.where(row == 0, across >> 6, across & 63).astype(f32)
    consts_ref[8:16, :] = jnp.full((8, 128), scale_ref[0], f32)
    consts_ref[16:24, :] = jnp.full((8, 128), bias_ref[0], f32)


def project(
    where_ref, sort_ref, split_ref, w_ref, r0_ref, r1_ref, r2_ref, r3_ref, out_ref, feat_ref
):
    sort = sort_ref[...]
    low = split_ref[0:192, :]
    high = split_ref[192:384, :]
    weights = [[], []]
    for half in range(2):
        some = w_ref[16 * half : 16 * half + 16]
        main = jnp.concatenate(
            [some[:, 0:24].reshape(384, 128), some[:, 24:48].reshape(384, 128)], axis=1
        )
        tail = some[:, 48:56].reshape(128, 128)
        main = jnp.dot(sort, main, preferred_element_type=f32).astype(bf16)
        low_tail = jnp.dot(low, tail, preferred_element_type=f32)
        high_tail = jnp.dot(high, tail, preferred_element_type=f32)
        for which in range(2):
            at = 64 * which
            tail = low_tail[:, at : at + 32] + high_tail[:, at + 32 : at + 64]
            tail = tail.astype(bf16)
            weights[which].append(
                jnp.concatenate([main[192 * which : 192 * which + 192]] + [tail] * 4, axis=1)
            )
    y = where_ref[3]
    for k, ref in enumerate((r0_ref, r1_ref, r2_ref, r3_ref)):
        feat_ref[(y - k) & 3] = ref[...]
    parts = []
    for which in range(2):
        rows = jnp.concatenate(
            [feat_ref[s, 16 * which : 16 * which + 16, :] for s in range(4)], axis=0
        )
        part = jnp.dot(rows[:, 0:192], weights[which][0], preferred_element_type=f32)
        parts.append(
            part + jnp.dot(rows[:, 192:384], weights[which][1], preferred_element_type=f32)
        )
    for y in range(4):
        rows = jnp.concatenate([part[16 * y : 16 * y + 16] for part in parts], axis=0)
        tail = jnp.concatenate(
            [rows[8 * g : 8 * g + 8, 256 + 32 * g : 288 + 32 * g] for g in range(4)], axis=1
        )
        block = jnp.concatenate([rows[:, 0:128], rows[:, 128:256], tail], axis=0).astype(bf16)
        for m in range(2):
            out_ref[2 * y + m] = block


def combine(got_ref, out_ref):
    for m in range(2):
        pre = got_ref[m].astype(f32)
        for part in range(1, 4):
            pre = pre + got_ref[2 * part + m].astype(f32)
        out_ref[m] = pre


def embed(got_ref, consts_ref, own_ref):
    total = jnp.zeros((32, 1), f32)
    tiles = []
    tails = []
    for col in range(4):
        pre = got_ref[2 * (col % 2) + col // 2]
        tiles += [pre[0:32], pre[32:64]]
        last = pre[64:72]
        tails.append(
            jnp.concatenate([last[:, 32 * g : 32 * g + 32] for g in range(4)], axis=0)
        )
    tiles.append(jnp.concatenate(tails, axis=1))
    for pre in tiles:
        total = total + jnp.sum(pre * pre, axis=1, keepdims=True)
    norm = lax.rsqrt(total + epsilon)
    for t, pre in enumerate(tiles):
        own_ref[32 * t : 32 * t + 32, :] = (pre * norm).astype(bf16)
    own_ref[288:296, :] = consts_ref[0:8, :].astype(bf16)


def choose(where_ref, own_ref, other_ref, out_ref, two_ref):
    z = where_ref[1]
    m = where_ref[2]
    two_ref[0] = own_ref[...]
    two_ref[1] = other_ref[...]
    middle = (m == 1) | (m == 2)
    for to in range(8):
        other_img = middle | ((m == 0) & (z >= to)) | ((m == 3) & (z < to))
        other_txt = middle | ((m == 0) & (z > to)) | ((m == 3) & (z <= to))
        img = jnp.where(other_img, 1, 0)
        txt = jnp.where(other_txt, 1, 0)
        for t in range(9):
            out_ref[to, 32 * t : 32 * t + 16, :] = two_ref[img, 32 * t : 32 * t + 16, :]
            out_ref[to, 32 * t + 16 : 32 * t + 32, :] = two_ref[
                txt, 32 * t + 16 : 32 * t + 32, :
            ]
        out_ref[to, 288:296, :] = two_ref[img, 288:296, :]


def score(where_ref, consts_ref, pair_ref, own_ref, got_ref, out_ref):
    octet = where_ref[0]
    z = where_ref[1]
    m = where_ref[2]
    scale = jnp.exp(consts_ref[8:9, :])
    scale_one = scale[:, 0:1]
    offset = consts_ref[16:17, :]

    def window(at):
        return jnp.concatenate(
            [
                jnp.concatenate(
                    [got_ref[k, 32 * t + at : 32 * t + at + 16, :] for k in range(8)], axis=0
                )
                for t in range(9)
            ],
            axis=1,
        )

    def mine(at):
        return jnp.concatenate(
            [own_ref[32 * t + at : 32 * t + at + 16, :] for t in range(9)], axis=1
        )

    imgs = window(0)
    txts = window(16)
    codes = got_ref[0, 288:296, :].astype(f32)
    for k in range(1, 8):
        codes = codes + got_ref[k, 288:296, :].astype(f32)
    pair_window = codes[0:1] * 64.0 + codes[1:2]
    lane = lax.broadcasted_iota(jnp.int32, (16, 128), 1)
    row = lax.broadcasted_iota(jnp.int32, (16, 128), 0)
    there = lane >> 4
    behind = jnp.where(there > z, -2, 0)
    ahead = jnp.where(there > z, 0, 2)
    delta = jnp.where(m == 0, behind, jnp.where(m == 3, ahead, jnp.where(m == 1, -1, 1)))
    block = (8 * (octet + delta) + there) & 127
    text_index = block * 16 + (lane & 15)
    match_img = pair_ref[...] == text_index
    own_text = (octet * 8 + z) * 16 + row
    match_txt = pair_window == own_text.astype(f32)

    def grads(own, window, match):
        scores = lax.dot_general(own, window, (((1,), (1,)), ((), ())), preferred_element_type=f32)
        logits = scale * scores + offset
        label = jnp.where(match, 1.0, -1.0)
        coef = (-label / (1.0 + jnp.exp(label * logits))).astype(bf16)
        return scale_one * jnp.dot(coef, window, preferred_element_type=f32)

    image_part = grads(mine(0), txts, match_img)
    text_part = grads(mine(16), imgs, match_txt)
    for to in range(4):
        rows = text_part[4 * to : 4 * to + 4]
        at = 1024 + 32 * to
        pieces = [
            image_part[:, 256 * to : 256 * to + 128],
            image_part[:, 256 * to + 128 : 256 * to + 256],
        ]
        pieces += [rows[:, 128 * t : 128 * t + 128] for t in range(9)]
        pieces.append(
            jnp.concatenate(
                [image_part[4 * g : 4 * g + 4, at : at + 32] for g in range(4)], axis=1
            )
        )
        out_ref[to] = jnp.concatenate(pieces, axis=0).astype(bf16)


def finish(got_ref, image_ref, text_ref):
    total = got_ref[0].astype(f32)
    for k in range(1, 4):
        total = total + got_ref[k].astype(f32)
    image_ref[:, 0:128] = total[0:16]
    image_ref[:, 128:256] = total[16:32]
    image_ref[:, 256:288] = jnp.concatenate(
        [total[68:72, 32 * g : 32 * g + 32] for g in range(4)], axis=0
    )
    pieces = []
    for c in range(4):
        pieces += [total[32 + 8 * c : 36 + 8 * c], total[36 + 8 * c : 40 + 8 * c]]
        pieces.append(total[64:68, 32 * c : 32 * c + 32])
    text_ref[...] = jnp.concatenate(pieces, axis=1)


def exchange(value, axes):
    return lax.all_to_all(value, axes, split_axis=0, concat_axis=0, tiled=True)


def local(img_feat, txt_feat, w_img, w_txt, pair_index, log_scale, bias):
    x, y, z = (lax.axis_index(a) for a in BATCH)
    m = lax.axis_index(MP)
    octet = 4 * x + y
    where = jnp.stack([octet, z, m, y]).astype(jnp.int32)

    sent = call(
        pack,
        jax.ShapeDtypeStruct((32, 56, 128), bf16),
        [pltpu.VMEM((12, 288), bf16), pltpu.VMEM((12, 288), bf16), pltpu.SemaphoreType.DMA((2,))],
        w_img,
        w_txt,
        hbm=(0, 1),
        vmem=60,
    )
    weights = exchange(sent, ("x", "z"))

    feats = jnp.concatenate([img_feat, txt_feat], axis=0).reshape(32, 4, 4, 96)
    feats = feats.transpose(2, 0, 1, 3).reshape(4, 32, 384)
    received = [lax.dynamic_index_in_dim(feats, y, 0, keepdims=False)]
    for k in range(1, 4):
        chosen = lax.dynamic_index_in_dim(feats, (y + k) % 4, 0, keepdims=False)
        received.append(
            lax.ppermute(chosen, "y", [(s, (s + k) % 4) for s in range(4)])
        )

    sort, split, pairs, consts = call(
        setup,
        (
            jax.ShapeDtypeStruct((384, 384), bf16),
            jax.ShapeDtypeStruct((384, 128), bf16),
            jax.ShapeDtypeStruct((16, 128), jnp.int32),
            jax.ShapeDtypeStruct((24, 128), f32),
        ),
        [],
        where,
        pair_index,
        log_scale,
        bias,
        smem=(0, 1, 2, 3),
    )

    sent = call(
        project,
        jax.ShapeDtypeStruct((8, 72, 128), bf16),
        [pltpu.VMEM((4, 32, 384), bf16)],
        where,
        sort,
        split,
        weights,
        *received,
        smem=(0,),
    )
    got = exchange(sent, ("y", "m0"))
    half = call(combine, jax.ShapeDtypeStruct((2, 72, 128), f32), [], got)
    got = lax.all_gather(half, "m1", axis=0, tiled=True)
    own = call(embed, jax.ShapeDtypeStruct((296, 128), bf16), [], got, consts)

    moves = []
    for s in range(512):
        o, rest = divmod(s, 32)
        moves.append((s, 32 * ((o - DELTA[rest % 4]) % 16) + rest))
    other = lax.ppermute(own, BATCH + MP, moves)
    sent = call(
        choose,
        jax.ShapeDtypeStruct((8, 296, 128), bf16),
        [pltpu.VMEM((2, 296, 128), bf16)],
        where,
        own,
        other,
        smem=(0,),
    )
    got = exchange(sent, "z")
    sent = call(
        score,
        jax.ShapeDtypeStruct((4, 72, 128), bf16),
        [],
        where,
        consts,
        pairs,
        own,
        got,
        smem=(0,),
    )
    got = exchange(sent, MP)
    return call(
        finish,
        (jax.ShapeDtypeStruct((16, 288), f32), jax.ShapeDtypeStruct((4, 1152), f32)),
        [],
        got,
    )


def solution(mesh):
    finer = Mesh(mesh.devices.reshape(4, 4, 8, 2, 2), BATCH + MP)
    in_specs = (P(BATCH, None), P(BATCH, None), P(BATCH, MP), P(BATCH, MP), P(BATCH), P(), P())
    out_specs = (P(BATCH, MP), P(BATCH + MP, None))

    return jax.shard_map(local, mesh=finer, in_specs=in_specs, out_specs=out_specs, check_vma=False)
```

```python
import jax
import jax.numpy as jnp
from jax import lax
from jax.experimental import pallas as pl
from jax.experimental.pallas import tpu as pltpu
from jax.sharding import Mesh
from jax.sharding import PartitionSpec as P


BATCH = ("x", "y", "z")
MP = ("m0", "m1")
bf16 = jnp.bfloat16
f32 = jnp.float32
epsilon = 1e-06
DELTA = (-1, -2, 1, 2)


def call(body, out_shape, scratch, *args, smem=(), hbm=(), vmem=16):
    spaces = [
        pltpu.SMEM if k in smem else pltpu.HBM if k in hbm else pltpu.VMEM for k in range(len(args))
    ]
    specs = [pl.BlockSpec(memory_space=space) for space in spaces]
    outs = jax.tree.map(lambda _: pl.BlockSpec(memory_space=pltpu.VMEM), out_shape)
    return pl.pallas_call(
        body, out_shape=out_shape, in_specs=specs, out_specs=outs, scratch_shapes=scratch,
        compiler_params=pltpu.CompilerParams(vmem_limit_bytes=vmem << 20),
    )(*args)


def pack(
    where_ref, w_img_ref, w_txt_ref, img_ref, txt_ref, pair_ref,
    out_ref, c0_ref, c1_ref, c2_ref, c3_ref, info_ref,
    w_img, w_txt, img, txt, pair, feats, sems,
):
    moves = ((w_img_ref, w_img), (w_txt_ref, w_txt), (img_ref, img), (txt_ref, txt))
    moves += ((pair_ref, pair),)
    copies = [pltpu.make_async_copy(a, b, sems.at[k]) for k, (a, b) in enumerate(moves)]
    for copy in copies:
        copy.start()
    for copy in copies:
        copy.wait()
    both = jnp.concatenate([w_img[...].astype(f32), w_txt[...].astype(f32)], axis=0)
    tail = jnp.concatenate([both[6 * g : 6 * g + 6, 256:288] for g in range(4)], axis=1)
    rows = [both[:, 0:128], both[:, 128:256], tail, jnp.zeros((2, 128), f32)]
    rows = jnp.concatenate(rows, axis=0).astype(bf16)
    for k in range(out_ref.shape[0]):
        out_ref[k] = rows
    for y in range(4):
        for which, feat in enumerate((img, txt)):
            for k in range(4):
                at = 384 * k + 96 * y
                feats[y, 16 * which : 16 * which + 16, 96 * k : 96 * k + 96] = feat[
                    :, at : at + 96
                ]
    for k, ref in enumerate((c0_ref, c1_ref, c2_ref, c3_ref)):
        ref[...] = feats[(where_ref[3] + k) & 3]
    row = lax.broadcasted_iota(jnp.int32, (16, 128), 0)
    lane = lax.broadcasted_iota(jnp.int32, (8, 128), 1) & 15
    down = jnp.zeros((16, 128), jnp.int32)
    across = jnp.zeros((8, 128), jnp.int32)
    for k in range(16):
        down = jnp.where(row == k, pair[k], down)
        across = jnp.where(lane == k, pair[k], across)
    info_ref[0:16, :] = down.astype(f32)
    info_ref[16:24, :] = across.astype(f32)


def setup(where_ref, info_ref, scalars_ref, sort_ref, split_ref, pairs_ref, consts_ref):
    r = lax.broadcasted_iota(jnp.int32, (384, 384), 0)
    c = lax.broadcasted_iota(jnp.int32, (384, 384), 1)
    second = r >= 192
    k = jnp.where(second, r - 192, r)
    source = k + 12 * ((k * 171) >> 11) + jnp.where(second, 12, 0)
    sort_ref[...] = jnp.where(c == source, 1.0, 0.0).astype(bf16)
    k = lax.broadcasted_iota(jnp.int32, (192, 128), 0)
    c = lax.broadcasted_iota(jnp.int32, (192, 128), 1)
    group = (k * 171) >> 11
    inner = k - 12 * group
    low = (inner < 6) & (c == 8 * group + inner)
    high = (inner >= 6) & (c == 8 * group + inner - 6)
    split_ref[0:192, :] = jnp.where(low, 1.0, 0.0).astype(bf16)
    split_ref[192:384, :] = jnp.where(high, 1.0, 0.0).astype(bf16)
    pairs_ref[...] = info_ref[0:16, :].astype(jnp.int32)
    row = lax.broadcasted_iota(jnp.int32, (8, 128), 0)
    lane = lax.broadcasted_iota(jnp.int32, (8, 128), 1)
    across = info_ref[16:24, :].astype(jnp.int32)
    across = jnp.where((lane >> 4) == where_ref[1], across, 0)
    consts_ref[0:8, :] = jnp.where(row == 0, across >> 6, across & 63).astype(f32)
    consts_ref[8:24, :] = scalars_ref[...]


def project(
    where_ref, sort_ref, split_ref, w_ref, r0_ref, r1_ref, r2_ref, r3_ref, out_ref, feat_ref
):
    sort = sort_ref[...]
    low = split_ref[0:192, :]
    high = split_ref[192:384, :]
    weights = [[], []]
    for half in range(2):
        some = w_ref[16 * half : 16 * half + 16]
        main = jnp.concatenate(
            [some[:, 0:24].reshape(384, 128), some[:, 24:48].reshape(384, 128)], axis=1
        )
        tail = some[:, 48:56].reshape(128, 128)
        main = jnp.dot(sort, main, preferred_element_type=f32).astype(bf16)
        low_tail = jnp.dot(low, tail, preferred_element_type=f32)
        high_tail = jnp.dot(high, tail, preferred_element_type=f32)
        for which in range(2):
            at = 64 * which
            tail = low_tail[:, at : at + 32] + high_tail[:, at + 32 : at + 64]
            tail = tail.astype(bf16)
            weights[which].append(
                jnp.concatenate([main[192 * which : 192 * which + 192]] + [tail] * 4, axis=1)
            )
    y = where_ref[3]
    for k, ref in enumerate((r0_ref, r1_ref, r2_ref, r3_ref)):
        feat_ref[(y - k) & 3] = ref[...]
    parts = []
    for which in range(2):
        rows = jnp.concatenate(
            [feat_ref[s, 16 * which : 16 * which + 16, :] for s in range(4)], axis=0
        )
        part = jnp.dot(rows[:, 0:192], weights[which][0], preferred_element_type=f32)
        parts.append(
            part + jnp.dot(rows[:, 192:384], weights[which][1], preferred_element_type=f32)
        )
    for y in range(4):
        rows = jnp.concatenate([part[16 * y : 16 * y + 16] for part in parts], axis=0)
        tail = jnp.concatenate(
            [rows[8 * g : 8 * g + 8, 256 + 32 * g : 288 + 32 * g] for g in range(4)], axis=1
        )
        block = jnp.concatenate([rows[:, 0:128], rows[:, 128:256], tail], axis=0).astype(bf16)
        for m in range(2):
            out_ref[2 * y + m] = block


def combine(got_ref, out_ref):
    for m in range(2):
        pre = got_ref[m].astype(f32)
        for part in range(1, 4):
            pre = pre + got_ref[2 * part + m].astype(f32)
        out_ref[m] = pre


def embed(got_ref, consts_ref, own_ref):
    total = jnp.zeros((32, 1), f32)
    tiles = []
    tails = []
    for col in range(4):
        pre = got_ref[2 * (col % 2) + col // 2]
        tiles += [pre[0:32], pre[32:64]]
        last = pre[64:72]
        tails.append(
            jnp.concatenate([last[:, 32 * g : 32 * g + 32] for g in range(4)], axis=0)
        )
    tiles.append(jnp.concatenate(tails, axis=1))
    for pre in tiles:
        total = total + jnp.sum(pre * pre, axis=1, keepdims=True)
    norm = lax.rsqrt(total + epsilon)
    for t, pre in enumerate(tiles):
        own_ref[32 * t : 32 * t + 32, :] = (pre * norm).astype(bf16)
    own_ref[288:296, :] = consts_ref[0:8, :].astype(bf16)


def choose(where_ref, own_ref, other_ref, out_ref, two_ref):
    z = where_ref[1]
    m = where_ref[2]
    two_ref[0] = own_ref[...]
    two_ref[1] = other_ref[...]
    near = (m == 0) | (m == 2)
    for to in range(8):
        other_img = near | ((m == 1) & (z >= to)) | ((m == 3) & (z < to))
        other_txt = near | ((m == 1) & (z > to)) | ((m == 3) & (z <= to))
        img = jnp.where(other_img, 1, 0)
        txt = jnp.where(other_txt, 1, 0)
        for t in range(9):
            out_ref[to, 32 * t : 32 * t + 16, :] = two_ref[img, 32 * t : 32 * t + 16, :]
            out_ref[to, 32 * t + 16 : 32 * t + 32, :] = two_ref[
                txt, 32 * t + 16 : 32 * t + 32, :
            ]
        out_ref[to, 288:296, :] = two_ref[img, 288:296, :]


def score(where_ref, consts_ref, pair_ref, own_ref, got_ref, out_ref):
    octet = where_ref[0]
    z = where_ref[1]
    m = where_ref[2]
    scale = consts_ref[8:9, :]
    scale_one = scale[:, 0:1]
    offset = consts_ref[16:17, :]

    def window(at):
        return jnp.concatenate(
            [
                jnp.concatenate(
                    [got_ref[k, 32 * t + at : 32 * t + at + 16, :] for k in range(8)], axis=0
                )
                for t in range(9)
            ],
            axis=1,
        )

    def mine(at):
        return jnp.concatenate(
            [own_ref[32 * t + at : 32 * t + at + 16, :] for t in range(9)], axis=1
        )

    imgs = window(0)
    txts = window(16)
    codes = got_ref[0, 288:296, :].astype(f32)
    for k in range(1, 8):
        codes = codes + got_ref[k, 288:296, :].astype(f32)
    pair_window = codes[0:1] * 64.0 + codes[1:2]
    lane = lax.broadcasted_iota(jnp.int32, (16, 128), 1)
    row = lax.broadcasted_iota(jnp.int32, (16, 128), 0)
    there = lane >> 4
    behind = jnp.where(there > z, -2, 0)
    ahead = jnp.where(there > z, 0, 2)
    delta = jnp.where(m == 1, behind, jnp.where(m == 3, ahead, m - 1))
    block = (8 * (octet + delta) + there) & 127
    text_index = block * 16 + (lane & 15)
    match_img = pair_ref[...] == text_index
    own_text = (octet * 8 + z) * 16 + row
    match_txt = pair_window == own_text.astype(f32)

    def grads(own, window, match):
        scores = lax.dot_general(own, window, (((1,), (1,)), ((), ())), preferred_element_type=f32)
        logits = scale * scores + offset
        label = jnp.where(match, 1.0, -1.0)
        coef = (-label / (1.0 + jnp.exp(label * logits))).astype(bf16)
        return scale_one * jnp.dot(coef, window, preferred_element_type=f32)

    image_part = grads(mine(0), txts, match_img)
    text_part = grads(mine(16), imgs, match_txt)
    for to in range(4):
        rows = text_part[4 * to : 4 * to + 4]
        at = 1024 + 32 * to
        pieces = [
            image_part[:, 256 * to : 256 * to + 128],
            image_part[:, 256 * to + 128 : 256 * to + 256],
        ]
        pieces += [rows[:, 128 * t : 128 * t + 128] for t in range(9)]
        pieces.append(
            jnp.concatenate(
                [image_part[4 * g : 4 * g + 4, at : at + 32] for g in range(4)], axis=1
            )
        )
        out_ref[to] = jnp.concatenate(pieces, axis=0).astype(bf16)


def finish(got_ref, image_ref, text_ref):
    total = got_ref[0].astype(f32)
    for k in range(1, 4):
        total = total + got_ref[k].astype(f32)
    image_ref[:, 0:128] = total[0:16]
    image_ref[:, 128:256] = total[16:32]
    image_ref[:, 256:288] = jnp.concatenate(
        [total[68:72, 32 * g : 32 * g + 32] for g in range(4)], axis=0
    )
    pieces = []
    for c in range(4):
        pieces += [total[32 + 8 * c : 36 + 8 * c], total[36 + 8 * c : 40 + 8 * c]]
        pieces.append(total[64:68, 32 * c : 32 * c + 32])
    text_ref[...] = jnp.concatenate(pieces, axis=1)


def exchange(value, axes):
    return lax.all_to_all(value, axes, split_axis=0, concat_axis=0, tiled=True)


def local(img_feat, txt_feat, w_img, w_txt, pair_index, log_scale, bias):
    x, y, z = (lax.axis_index(a) for a in BATCH)
    m = lax.axis_index(MP)
    octet = 4 * x + y
    where = jnp.stack([octet, z, m, y]).astype(jnp.int32)

    sent, *chosen, info = call(
        pack,
        (jax.ShapeDtypeStruct((32, 56, 128), bf16),)
        + (jax.ShapeDtypeStruct((32, 384), bf16),) * 4
        + (jax.ShapeDtypeStruct((24, 128), f32),),
        [pltpu.VMEM((12, 288), bf16)] * 2
        + [pltpu.VMEM((16, 1536), bf16)] * 2
        + [pltpu.SMEM((16,), jnp.int32)]
        + [pltpu.VMEM((4, 32, 384), bf16), pltpu.SemaphoreType.DMA((5,))],
        where,
        w_img,
        w_txt,
        img_feat,
        txt_feat,
        pair_index,
        smem=(0,),
        hbm=(1, 2, 3, 4, 5),
        vmem=60,
    )
    weights = exchange(sent, ("x", "z"))

    received = [chosen[0]]
    for k in range(1, 4):
        received.append(
            lax.ppermute(chosen[k], "y", [(s, (s + k) % 4) for s in range(4)])
        )

    row = lax.broadcasted_iota(jnp.int32, (16, 128), 0)
    scalars = jnp.where(row < 8, jnp.exp(log_scale[0]), bias[0])
    sort, split, pairs, consts = call(
        setup,
        (
            jax.ShapeDtypeStruct((384, 384), bf16),
            jax.ShapeDtypeStruct((384, 128), bf16),
            jax.ShapeDtypeStruct((16, 128), jnp.int32),
            jax.ShapeDtypeStruct((24, 128), f32),
        ),
        [],
        where,
        info,
        scalars,
        smem=(0,),
    )

    sent = call(
        project,
        jax.ShapeDtypeStruct((8, 72, 128), bf16),
        [pltpu.VMEM((4, 32, 384), bf16)],
        where,
        sort,
        split,
        weights,
        *received,
        smem=(0,),
    )
    got = exchange(sent, ("y", "m0"))
    half = call(combine, jax.ShapeDtypeStruct((2, 72, 128), f32), [], got)
    got = lax.all_gather(half, "m1", axis=0, tiled=True)
    own = call(embed, jax.ShapeDtypeStruct((296, 128), bf16), [], got, consts)

    moves = []
    for s in range(512):
        o, rest = divmod(s, 32)
        moves.append((s, 32 * ((o - DELTA[rest % 4]) % 16) + rest))
    other = lax.ppermute(own, BATCH + MP, moves)
    sent = call(
        choose,
        jax.ShapeDtypeStruct((8, 296, 128), bf16),
        [pltpu.VMEM((2, 296, 128), bf16)],
        where,
        own,
        other,
        smem=(0,),
    )
    got = exchange(sent, "z")
    sent = call(
        score,
        jax.ShapeDtypeStruct((4, 72, 128), bf16),
        [],
        where,
        consts,
        pairs,
        own,
        got,
        smem=(0,),
    )
    got = exchange(sent, MP)
    return call(
        finish,
        (jax.ShapeDtypeStruct((16, 288), f32), jax.ShapeDtypeStruct((4, 1152), f32)),
        [],
        got,
    )


def solution(mesh):
    finer = Mesh(mesh.devices.reshape(4, 4, 8, 2, 2), BATCH + MP)
    in_specs = (P(BATCH, None), P(BATCH, None), P(BATCH, MP), P(BATCH, MP), P(BATCH), P(), P())
    out_specs = (P(BATCH, MP), P(BATCH + MP, None))

    return jax.shard_map(local, mesh=finer, in_specs=in_specs, out_specs=out_specs, check_vma=False)
```

```python
import jax
import jax.numpy as jnp
from jax import lax
from jax.experimental import pallas as pl
from jax.experimental.pallas import tpu as pltpu
from jax.sharding import Mesh
from jax.sharding import PartitionSpec as P


X = ("x1", "x0")
Z = ("z2", "z1", "z0")
BATCH = X + ("y",) + Z
SPREAD = ("z0", "x0", "z1", "x1", "z2")
MP = ("m0", "m1")
bf16 = jnp.bfloat16
f32 = jnp.float32
epsilon = 1e-06
DELTA = (-1, -2, 1, 2)


def call(body, out_shape, scratch, *args, smem=(), hbm=(), vmem=16):
    spaces = [
        pltpu.SMEM if k in smem else pltpu.HBM if k in hbm else pltpu.VMEM for k in range(len(args))
    ]
    specs = [pl.BlockSpec(memory_space=space) for space in spaces]
    outs = jax.tree.map(lambda _: pl.BlockSpec(memory_space=pltpu.VMEM), out_shape)
    return pl.pallas_call(
        body, out_shape=out_shape, in_specs=specs, out_specs=outs, scratch_shapes=scratch,
        compiler_params=pltpu.CompilerParams(vmem_limit_bytes=vmem << 20),
    )(*args)


def pack(img_ref, txt_ref, out_ref, img, txt, sems):
    copies = [
        pltpu.make_async_copy(img_ref, img, sems.at[0]),
        pltpu.make_async_copy(txt_ref, txt, sems.at[1]),
    ]
    for copy in copies:
        copy.start()
    for copy in copies:
        copy.wait()
    both = jnp.concatenate([img[...].astype(f32), txt[...].astype(f32)], axis=0)
    tail = jnp.concatenate([both[6 * g : 6 * g + 6, 256:288] for g in range(4)], axis=1)
    rows = [both[:, 0:128], both[:, 128:256], tail, jnp.zeros((2, 128), f32)]
    rows = jnp.concatenate(rows, axis=0).astype(bf16)
    for k in range(out_ref.shape[0]):
        out_ref[k] = rows


def setup(where_ref, pair_ref, sort_ref, split_ref, pairs_ref, codes_ref):
    r = lax.broadcasted_iota(jnp.int32, (384, 384), 0)
    c = lax.broadcasted_iota(jnp.int32, (384, 384), 1)
    second = r >= 192
    k = jnp.where(second, r - 192, r)
    source = k + 12 * ((k * 171) >> 11) + jnp.where(second, 12, 0)
    sort_ref[...] = jnp.where(c == source, 1.0, 0.0).astype(bf16)
    k = lax.broadcasted_iota(jnp.int32, (192, 128), 0)
    c = lax.broadcasted_iota(jnp.int32, (192, 128), 1)
    group = (k * 171) >> 11
    inner = k - 12 * group
    low = (inner < 6) & (c == 8 * group + inner)
    high = (inner >= 6) & (c == 8 * group + inner - 6)
    split_ref[0:192, :] = jnp.where(low, 1.0, 0.0).astype(bf16)
    split_ref[192:384, :] = jnp.where(high, 1.0, 0.0).astype(bf16)
    row = lax.broadcasted_iota(jnp.int32, (16, 128), 0)
    lane = lax.broadcasted_iota(jnp.int32, (8, 128), 1)
    down = jnp.zeros((16, 128), jnp.int32)
    across = jnp.zeros((8, 128), jnp.int32)
    for k in range(16):
        down = jnp.where(row == k, pair_ref[k], down)
        across = jnp.where(lane == 16 * where_ref[1] + k, pair_ref[k], across)
    pairs_ref[...] = down
    row = lax.broadcasted_iota(jnp.int32, (8, 128), 0)
    codes_ref[...] = jnp.where(row == 0, across >> 6, across & 63).astype(f32)


def project(
    where_ref, sort_ref, split_ref, w_ref, r0_ref, r1_ref, r2_ref, r3_ref, out_ref, feat_ref
):
    sort = sort_ref[...]
    low = split_ref[0:192, :]
    high = split_ref[192:384, :]
    weights = [[], []]
    for half in range(2):
        places = []
        for q in range(16 * half, 16 * half + 16):
            x1, x0, z2, z1, z0 = (q >> 4) & 1, (q >> 3) & 1, (q >> 2) & 1, (q >> 1) & 1, q & 1
            places.append(16 * z0 + 8 * x0 + 4 * z1 + 2 * x1 + z2)
        some = jnp.stack([w_ref[place] for place in places], axis=0)
        main = jnp.concatenate(
            [some[:, 0:24].reshape(384, 128), some[:, 24:48].reshape(384, 128)], axis=1
        )
        tail = some[:, 48:56].reshape(128, 128)
        main = jnp.dot(sort, main, preferred_element_type=f32).astype(bf16)
        low_tail = jnp.dot(low, tail, preferred_element_type=f32)
        high_tail = jnp.dot(high, tail, preferred_element_type=f32)
        for which in range(2):
            at = 64 * which
            tail = low_tail[:, at : at + 32] + high_tail[:, at + 32 : at + 64]
            tail = tail.astype(bf16)
            weights[which].append(
                jnp.concatenate([main[192 * which : 192 * which + 192]] + [tail] * 4, axis=1)
            )
    y = where_ref[3]
    for k, ref in enumerate((r0_ref, r1_ref, r2_ref, r3_ref)):
        feat_ref[(y - k) & 3] = ref[...]
    parts = []
    for which in range(2):
        rows = jnp.concatenate(
            [feat_ref[s, 16 * which : 16 * which + 16, :] for s in range(4)], axis=0
        )
        part = jnp.dot(rows[:, 0:192], weights[which][0], preferred_element_type=f32)
        parts.append(
            part + jnp.dot(rows[:, 192:384], weights[which][1], preferred_element_type=f32)
        )
    for y in range(4):
        rows = jnp.concatenate([part[16 * y : 16 * y + 16] for part in parts], axis=0)
        tail = jnp.concatenate(
            [rows[8 * g : 8 * g + 8, 256 + 32 * g : 288 + 32 * g] for g in range(4)], axis=1
        )
        block = jnp.concatenate([rows[:, 0:128], rows[:, 128:256], tail], axis=0).astype(bf16)
        for m in range(2):
            out_ref[2 * y + m] = block


def combine(got_ref, out_ref):
    for m in range(2):
        pre = got_ref[m].astype(f32)
        for part in range(1, 4):
            pre = pre + got_ref[2 * part + m].astype(f32)
        out_ref[m] = pre


def embed(got_ref, codes_ref, own_ref):
    total = jnp.zeros((32, 1), f32)
    tiles = []
    tails = []
    for col in range(4):
        pre = got_ref[2 * (col % 2) + col // 2]
        tiles += [pre[0:32], pre[32:64]]
        last = pre[64:72]
        tails.append(
            jnp.concatenate([last[:, 32 * g : 32 * g + 32] for g in range(4)], axis=0)
        )
    tiles.append(jnp.concatenate(tails, axis=1))
    for pre in tiles:
        total = total + jnp.sum(pre * pre, axis=1, keepdims=True)
    norm = lax.rsqrt(total + epsilon)
    for t, pre in enumerate(tiles):
        own_ref[32 * t : 32 * t + 32, :] = (pre * norm).astype(bf16)
    own_ref[288:296, :] = codes_ref[...].astype(bf16)


def choose(where_ref, own_ref, other_ref, out_ref, two_ref):
    z = where_ref[1]
    m = where_ref[2]
    two_ref[0] = own_ref[...]
    two_ref[1] = other_ref[...]
    near = (m == 0) | (m == 2)
    for to in range(8):
        other_img = near | ((m == 1) & (z >= to)) | ((m == 3) & (z < to))
        other_txt = near | ((m == 1) & (z > to)) | ((m == 3) & (z <= to))
        img = jnp.where(other_img, 1, 0)
        txt = jnp.where(other_txt, 1, 0)
        for t in range(9):
            out_ref[to, 32 * t : 32 * t + 16, :] = two_ref[img, 32 * t : 32 * t + 16, :]
            out_ref[to, 32 * t + 16 : 32 * t + 32, :] = two_ref[
                txt, 32 * t + 16 : 32 * t + 32, :
            ]
        out_ref[to, 288:296, :] = two_ref[img, 288:296, :]


def score(where_ref, scalars_ref, pair_ref, own_ref, got_ref, out_ref):
    octet = where_ref[0]
    z = where_ref[1]
    m = where_ref[2]
    scale = scalars_ref[0:1, :]
    scale_one = scale[:, 0:1]
    offset = scalars_ref[8:9, :]

    def window(at):
        return jnp.concatenate(
            [
                jnp.concatenate(
                    [got_ref[k, 32 * t + at : 32 * t + at + 16, :] for k in range(8)], axis=0
                )
                for t in range(9)
            ],
            axis=1,
        )

    def mine(at):
        return jnp.concatenate(
            [own_ref[32 * t + at : 32 * t + at + 16, :] for t in range(9)], axis=1
        )

    imgs = window(0)
    txts = window(16)
    codes = got_ref[0, 288:296, :].astype(f32)
    for k in range(1, 8):
        codes = codes + got_ref[k, 288:296, :].astype(f32)
    pair_window = codes[0:1] * 64.0 + codes[1:2]
    lane = lax.broadcasted_iota(jnp.int32, (16, 128), 1)
    row = lax.broadcasted_iota(jnp.int32, (16, 128), 0)
    there = lane >> 4
    behind = jnp.where(there > z, -2, 0)
    ahead = jnp.where(there > z, 0, 2)
    delta = jnp.where(m == 1, behind, jnp.where(m == 3, ahead, m - 1))
    block = (8 * (octet + delta) + there) & 127
    text_index = block * 16 + (lane & 15)
    match_img = pair_ref[...] == text_index
    own_text = (octet * 8 + z) * 16 + row
    match_txt = pair_window == own_text.astype(f32)

    def grads(own, window, match):
        scores = lax.dot_general(own, window, (((1,), (1,)), ((), ())), preferred_element_type=f32)
        logits = scale * scores + offset
        label = jnp.where(match, 1.0, -1.0)
        coef = (-label / (1.0 + jnp.exp(label * logits))).astype(bf16)
        return scale_one * jnp.dot(coef, window, preferred_element_type=f32)

    image_part = grads(mine(0), txts, match_img)
    text_part = grads(mine(16), imgs, match_txt)
    for to in range(4):
        rows = text_part[4 * to : 4 * to + 4]
        at = 1024 + 32 * to
        pieces = [
            image_part[:, 256 * to : 256 * to + 128],
            image_part[:, 256 * to + 128 : 256 * to + 256],
        ]
        pieces += [rows[:, 128 * t : 128 * t + 128] for t in range(9)]
        pieces.append(
            jnp.concatenate(
                [image_part[4 * g : 4 * g + 4, at : at + 32] for g in range(4)], axis=1
            )
        )
        out_ref[to] = jnp.concatenate(pieces, axis=0).astype(bf16)


def finish(got_ref, image_ref, text_ref):
    total = got_ref[0].astype(f32)
    for k in range(1, 4):
        total = total + got_ref[k].astype(f32)
    image_ref[:, 0:128] = total[0:16]
    image_ref[:, 128:256] = total[16:32]
    image_ref[:, 256:288] = jnp.concatenate(
        [total[68:72, 32 * g : 32 * g + 32] for g in range(4)], axis=0
    )
    pieces = []
    for c in range(4):
        pieces += [total[32 + 8 * c : 36 + 8 * c], total[36 + 8 * c : 40 + 8 * c]]
        pieces.append(total[64:68, 32 * c : 32 * c + 32])
    text_ref[...] = jnp.concatenate(pieces, axis=1)


def exchange(value, axes):
    return lax.all_to_all(value, axes, split_axis=0, concat_axis=0, tiled=True)


def local(img_feat, txt_feat, w_img, w_txt, pair_index, log_scale, bias):
    x, y, z = (lax.axis_index(a) for a in (X, "y", Z))
    m = lax.axis_index(MP)
    octet = 4 * x + y
    where = jnp.stack([octet, z, m, y]).astype(jnp.int32)

    sent = call(
        pack,
        jax.ShapeDtypeStruct((32, 56, 128), bf16),
        [pltpu.VMEM((12, 288), bf16), pltpu.VMEM((12, 288), bf16), pltpu.SemaphoreType.DMA((2,))],
        w_img,
        w_txt,
        hbm=(0, 1),
        vmem=60,
    )
    weights = exchange(sent, SPREAD)

    feats = jnp.concatenate([img_feat, txt_feat], axis=0).reshape(32, 4, 4, 96)
    feats = feats.transpose(2, 0, 1, 3).reshape(4, 32, 384)
    received = [lax.dynamic_index_in_dim(feats, y, 0, keepdims=False)]
    for k in range(1, 4):
        chosen = lax.dynamic_index_in_dim(feats, (y + k) % 4, 0, keepdims=False)
        received.append(
            lax.ppermute(chosen, "y", [(s, (s + k) % 4) for s in range(4)])
        )

    sort, split, pairs, codes = call(
        setup,
        (
            jax.ShapeDtypeStruct((384, 384), bf16),
            jax.ShapeDtypeStruct((384, 128), bf16),
            jax.ShapeDtypeStruct((16, 128), jnp.int32),
            jax.ShapeDtypeStruct((8, 128), f32),
        ),
        [],
        where,
        pair_index,
        smem=(0, 1),
    )

    sent = call(
        project,
        jax.ShapeDtypeStruct((8, 72, 128), bf16),
        [pltpu.VMEM((4, 32, 384), bf16)],
        where,
        sort,
        split,
        weights,
        *received,
        smem=(0,),
    )
    got = exchange(sent, ("y", "m0"))
    half = call(combine, jax.ShapeDtypeStruct((2, 72, 128), f32), [], got)
    got = lax.all_gather(half, "m1", axis=0, tiled=True)
    own = call(embed, jax.ShapeDtypeStruct((296, 128), bf16), [], got, codes)

    moves = []
    for s in range(512):
        o, rest = divmod(s, 32)
        moves.append((s, 32 * ((o - DELTA[rest % 4]) % 16) + rest))
    own, log_scale, bias = lax.optimization_barrier((own, log_scale, bias))
    other = lax.ppermute(own, BATCH + MP, moves)
    row = lax.broadcasted_iota(jnp.int32, (16, 128), 0)
    scalars = jnp.where(row < 8, jnp.exp(log_scale[0]), bias[0])
    sent = call(
        choose,
        jax.ShapeDtypeStruct((8, 296, 128), bf16),
        [pltpu.VMEM((2, 296, 128), bf16)],
        where,
        own,
        other,
        smem=(0,),
    )
    got = exchange(sent, Z)
    sent = call(
        score,
        jax.ShapeDtypeStruct((4, 72, 128), bf16),
        [],
        where,
        scalars,
        pairs,
        own,
        got,
        smem=(0,),
    )
    got = exchange(sent, MP)
    return call(
        finish,
        (jax.ShapeDtypeStruct((16, 288), f32), jax.ShapeDtypeStruct((4, 1152), f32)),
        [],
        got,
    )


def solution(mesh):
    finer = Mesh(mesh.devices.reshape(2, 2, 4, 2, 2, 2, 2, 2), BATCH + MP)
    in_specs = (P(BATCH, None), P(BATCH, None), P(BATCH, MP), P(BATCH, MP), P(BATCH), P(), P())
    out_specs = (P(BATCH, MP), P(BATCH + MP, None))

    return jax.shard_map(local, mesh=finer, in_specs=in_specs, out_specs=out_specs, check_vma=False)
```

```python
import jax
import jax.numpy as jnp
from jax import lax
from jax.experimental import pallas as pl
from jax.experimental.pallas import tpu as pltpu
from jax.sharding import Mesh
from jax.sharding import PartitionSpec as P


X = ("x1", "x0")
Z = ("z2", "z1", "z0")
BATCH = X + ("y",) + Z
SPREAD = ("z0", "x0", "z1", "x1", "z2")
MP = ("m0", "m1")
bf16 = jnp.bfloat16
f32 = jnp.float32
epsilon = 1e-06
DELTA = (-1, -2, 1, 2)


def call(body, out_shape, scratch, *args, smem=(), hbm=(), out=pltpu.VMEM, vmem=16):
    spaces = [
        pltpu.SMEM if k in smem else pltpu.HBM if k in hbm else pltpu.VMEM for k in range(len(args))
    ]
    specs = [pl.BlockSpec(memory_space=space) for space in spaces]
    outs = jax.tree.map(lambda _: pl.BlockSpec(memory_space=out), out_shape)
    return pl.pallas_call(
        body, out_shape=out_shape, in_specs=specs, out_specs=outs, scratch_shapes=scratch,
        compiler_params=pltpu.CompilerParams(vmem_limit_bytes=vmem << 20),
    )(*args)


def pack(
    w_img_ref, w_txt_ref, img_ref, txt_ref, out_ref, c0_ref, c1_ref, c2_ref, c3_ref,
    w_img, w_txt, img, txt, rows, feats, in_sems, out_sems,
):
    moves = ((w_img_ref, w_img), (w_txt_ref, w_txt), (img_ref, img), (txt_ref, txt))
    reads = [pltpu.make_async_copy(a, b, in_sems.at[k]) for k, (a, b) in enumerate(moves)]
    for copy in reads:
        copy.start()
    for copy in reads[:2]:
        copy.wait()
    both = jnp.concatenate([w_img[...].astype(f32), w_txt[...].astype(f32)], axis=0)
    tail = jnp.concatenate([both[6 * g : 6 * g + 6, 256:288] for g in range(4)], axis=1)
    block = [both[:, 0:128], both[:, 128:256], tail, jnp.zeros((2, 128), f32)]
    block = jnp.concatenate(block, axis=0).astype(bf16)
    for k in range(8):
        rows[k] = block
    writes = [
        pltpu.make_async_copy(rows, out_ref.at[8 * k : 8 * k + 8], out_sems.at[k])
        for k in range(4)
    ]
    for copy in writes:
        copy.start()
    for copy in reads[2:]:
        copy.wait()
    for y in range(4):
        for which, feat in enumerate((img, txt)):
            for k in range(4):
                at = 384 * k + 96 * y
                feats[y, 16 * which : 16 * which + 16, 96 * k : 96 * k + 96] = feat[
                    :, at : at + 96
                ]
    here = lax.axis_index("y")
    more = [
        pltpu.make_async_copy(feats.at[(here + k) & 3], ref, out_sems.at[4 + k])
        for k, ref in enumerate((c0_ref, c1_ref, c2_ref, c3_ref))
    ]
    for copy in more:
        copy.start()
    for copy in writes + more:
        copy.wait()


def setup(
    where_ref, pair_ref, scale_ref, bias_ref, sort_ref, split_ref, pairs_ref, codes_ref, scalars_ref
):
    r = lax.broadcasted_iota(jnp.int32, (384, 384), 0)
    c = lax.broadcasted_iota(jnp.int32, (384, 384), 1)
    second = r >= 192
    k = jnp.where(second, r - 192, r)
    source = k + 12 * ((k * 171) >> 11) + jnp.where(second, 12, 0)
    sort_ref[...] = jnp.where(c == source, 1.0, 0.0).astype(bf16)
    k = lax.broadcasted_iota(jnp.int32, (192, 128), 0)
    c = lax.broadcasted_iota(jnp.int32, (192, 128), 1)
    group = (k * 171) >> 11
    inner = k - 12 * group
    low = (inner < 6) & (c == 8 * group + inner)
    high = (inner >= 6) & (c == 8 * group + inner - 6)
    split_ref[0:192, :] = jnp.where(low, 1.0, 0.0).astype(bf16)
    split_ref[192:384, :] = jnp.where(high, 1.0, 0.0).astype(bf16)
    row = lax.broadcasted_iota(jnp.int32, (16, 128), 0)
    lane = lax.broadcasted_iota(jnp.int32, (8, 128), 1)
    down = jnp.zeros((16, 128), jnp.int32)
    across = jnp.zeros((8, 128), jnp.int32)
    for k in range(16):
        down = jnp.where(row == k, pair_ref[k], down)
        across = jnp.where(lane == 16 * where_ref[1] + k, pair_ref[k], across)
    pairs_ref[...] = down
    row = lax.broadcasted_iota(jnp.int32, (8, 128), 0)
    codes_ref[...] = jnp.where(row == 0, across >> 6, across & 63).astype(f32)
    scalars_ref[0:8, :] = jnp.exp(jnp.full((8, 128), scale_ref[0], f32))
    scalars_ref[8:16, :] = jnp.full((8, 128), bias_ref[0], f32)


def project(
    where_ref, sort_ref, split_ref, w_ref, r0_ref, r1_ref, r2_ref, r3_ref, out_ref, feat_ref
):
    sort = sort_ref[...]
    low = split_ref[0:192, :]
    high = split_ref[192:384, :]
    weights = [[], []]
    for half in range(2):
        places = []
        for q in range(16 * half, 16 * half + 16):
            x1, x0, z2, z1, z0 = (q >> 4) & 1, (q >> 3) & 1, (q >> 2) & 1, (q >> 1) & 1, q & 1
            places.append(16 * z0 + 8 * x0 + 4 * z1 + 2 * x1 + z2)
        some = jnp.stack([w_ref[place] for place in places], axis=0)
        main = jnp.concatenate(
            [some[:, 0:24].reshape(384, 128), some[:, 24:48].reshape(384, 128)], axis=1
        )
        tail = some[:, 48:56].reshape(128, 128)
        main = jnp.dot(sort, main, preferred_element_type=f32).astype(bf16)
        low_tail = jnp.dot(low, tail, preferred_element_type=f32)
        high_tail = jnp.dot(high, tail, preferred_element_type=f32)
        for which in range(2):
            at = 64 * which
            tail = low_tail[:, at : at + 32] + high_tail[:, at + 32 : at + 64]
            tail = tail.astype(bf16)
            weights[which].append(
                jnp.concatenate([main[192 * which : 192 * which + 192]] + [tail] * 4, axis=1)
            )
    y = where_ref[3]
    for k, ref in enumerate((r0_ref, r1_ref, r2_ref, r3_ref)):
        feat_ref[(y - k) & 3] = ref[...]
    parts = []
    for which in range(2):
        rows = jnp.concatenate(
            [feat_ref[s, 16 * which : 16 * which + 16, :] for s in range(4)], axis=0
        )
        part = jnp.dot(rows[:, 0:192], weights[which][0], preferred_element_type=f32)
        parts.append(
            part + jnp.dot(rows[:, 192:384], weights[which][1], preferred_element_type=f32)
        )
    for y in range(4):
        rows = jnp.concatenate([part[16 * y : 16 * y + 16] for part in parts], axis=0)
        tail = jnp.concatenate(
            [rows[8 * g : 8 * g + 8, 256 + 32 * g : 288 + 32 * g] for g in range(4)], axis=1
        )
        block = jnp.concatenate([rows[:, 0:128], rows[:, 128:256], tail], axis=0).astype(bf16)
        for m in range(2):
            out_ref[2 * y + m] = block


def combine(got_ref, out_ref):
    for m in range(2):
        pre = got_ref[m].astype(f32)
        for part in range(1, 4):
            pre = pre + got_ref[2 * part + m].astype(f32)
        out_ref[m] = pre


def embed(got_ref, codes_ref, own_ref):
    total = jnp.zeros((32, 1), f32)
    tiles = []
    tails = []
    for col in range(4):
        pre = got_ref[2 * (col % 2) + col // 2]
        tiles += [pre[0:32], pre[32:64]]
        last = pre[64:72]
        tails.append(
            jnp.concatenate([last[:, 32 * g : 32 * g + 32] for g in range(4)], axis=0)
        )
    tiles.append(jnp.concatenate(tails, axis=1))
    for pre in tiles:
        total = total + jnp.sum(pre * pre, axis=1, keepdims=True)
    norm = lax.rsqrt(total + epsilon)
    for t, pre in enumerate(tiles):
        own_ref[32 * t : 32 * t + 32, :] = (pre * norm).astype(bf16)
    own_ref[288:296, :] = codes_ref[...].astype(bf16)


def choose(where_ref, own_ref, other_ref, out_ref, two_ref):
    z = where_ref[1]
    m = where_ref[2]
    two_ref[0] = own_ref[...]
    two_ref[1] = other_ref[...]
    near = (m == 0) | (m == 2)
    for to in range(8):
        other_img = near | ((m == 1) & (z >= to)) | ((m == 3) & (z < to))
        other_txt = near | ((m == 1) & (z > to)) | ((m == 3) & (z <= to))
        img = jnp.where(other_img, 1, 0)
        txt = jnp.where(other_txt, 1, 0)
        for t in range(9):
            out_ref[to, 32 * t : 32 * t + 16, :] = two_ref[img, 32 * t : 32 * t + 16, :]
            out_ref[to, 32 * t + 16 : 32 * t + 32, :] = two_ref[
                txt, 32 * t + 16 : 32 * t + 32, :
            ]
        out_ref[to, 288:296, :] = two_ref[img, 288:296, :]


def score(where_ref, scalars_ref, pair_ref, own_ref, got_ref, out_ref):
    octet = where_ref[0]
    z = where_ref[1]
    m = where_ref[2]
    scale = scalars_ref[0:1, :]
    scale_one = scale[:, 0:1]
    offset = scalars_ref[8:9, :]

    def window(at):
        return jnp.concatenate(
            [
                jnp.concatenate(
                    [got_ref[k, 32 * t + at : 32 * t + at + 16, :] for k in range(8)], axis=0
                )
                for t in range(9)
            ],
            axis=1,
        )

    def mine(at):
        return jnp.concatenate(
            [own_ref[32 * t + at : 32 * t + at + 16, :] for t in range(9)], axis=1
        )

    imgs = window(0)
    txts = window(16)
    codes = got_ref[0, 288:296, :].astype(f32)
    for k in range(1, 8):
        codes = codes + got_ref[k, 288:296, :].astype(f32)
    pair_window = codes[0:1] * 64.0 + codes[1:2]
    lane = lax.broadcasted_iota(jnp.int32, (16, 128), 1)
    row = lax.broadcasted_iota(jnp.int32, (16, 128), 0)
    there = lane >> 4
    behind = jnp.where(there > z, -2, 0)
    ahead = jnp.where(there > z, 0, 2)
    delta = jnp.where(m == 1, behind, jnp.where(m == 3, ahead, m - 1))
    block = (8 * (octet + delta) + there) & 127
    text_index = block * 16 + (lane & 15)
    match_img = pair_ref[...] == text_index
    own_text = (octet * 8 + z) * 16 + row
    match_txt = pair_window == own_text.astype(f32)

    def grads(own, window, match):
        scores = lax.dot_general(own, window, (((1,), (1,)), ((), ())), preferred_element_type=f32)
        logits = scale * scores + offset
        label = jnp.where(match, 1.0, -1.0)
        coef = (-label / (1.0 + jnp.exp(label * logits))).astype(bf16)
        return scale_one * jnp.dot(coef, window, preferred_element_type=f32)

    image_part = grads(mine(0), txts, match_img)
    text_part = grads(mine(16), imgs, match_txt)
    for to in range(4):
        rows = text_part[4 * to : 4 * to + 4]
        at = 1024 + 32 * to
        pieces = [
            image_part[:, 256 * to : 256 * to + 128],
            image_part[:, 256 * to + 128 : 256 * to + 256],
        ]
        pieces += [rows[:, 128 * t : 128 * t + 128] for t in range(9)]
        pieces.append(
            jnp.concatenate(
                [image_part[4 * g : 4 * g + 4, at : at + 32] for g in range(4)], axis=1
            )
        )
        out_ref[to] = jnp.concatenate(pieces, axis=0).astype(bf16)


def finish(got_ref, image_ref, text_ref):
    total = got_ref[0].astype(f32)
    for k in range(1, 4):
        total = total + got_ref[k].astype(f32)
    image_ref[:, 0:128] = total[0:16]
    image_ref[:, 128:256] = total[16:32]
    image_ref[:, 256:288] = jnp.concatenate(
        [total[68:72, 32 * g : 32 * g + 32] for g in range(4)], axis=0
    )
    pieces = []
    for c in range(4):
        pieces += [total[32 + 8 * c : 36 + 8 * c], total[36 + 8 * c : 40 + 8 * c]]
        pieces.append(total[64:68, 32 * c : 32 * c + 32])
    text_ref[...] = jnp.concatenate(pieces, axis=1)


def exchange(value, axes):
    return lax.all_to_all(value, axes, split_axis=0, concat_axis=0, tiled=True)


def local(img_feat, txt_feat, w_img, w_txt, pair_index, log_scale, bias):
    x, y, z = (lax.axis_index(a) for a in (X, "y", Z))
    m = lax.axis_index(MP)
    octet = 4 * x + y
    where = jnp.stack([octet, z, m, y]).astype(jnp.int32)

    sent, *chosen = call(
        pack,
        (jax.ShapeDtypeStruct((32, 56, 128), bf16),)
        + (jax.ShapeDtypeStruct((32, 384), bf16),) * 4,
        [pltpu.VMEM((12, 288), bf16)] * 2
        + [pltpu.VMEM((16, 1536), bf16)] * 2
        + [pltpu.VMEM((8, 56, 128), bf16), pltpu.VMEM((4, 32, 384), bf16)]
        + [pltpu.SemaphoreType.DMA((4,)), pltpu.SemaphoreType.DMA((8,))],
        w_img,
        w_txt,
        img_feat,
        txt_feat,
        hbm=(0, 1, 2, 3),
        out=pltpu.HBM,
        vmem=60,
    )
    weights = exchange(sent, SPREAD)

    received = [chosen[0]]
    for k in range(1, 4):
        received.append(
            lax.ppermute(chosen[k], "y", [(s, (s + k) % 4) for s in range(4)])
        )

    sort, split, pairs, codes, scalars = call(
        setup,
        (
            jax.ShapeDtypeStruct((384, 384), bf16),
            jax.ShapeDtypeStruct((384, 128), bf16),
            jax.ShapeDtypeStruct((16, 128), jnp.int32),
            jax.ShapeDtypeStruct((8, 128), f32),
            jax.ShapeDtypeStruct((16, 128), f32),
        ),
        [],
        where,
        pair_index,
        log_scale,
        bias,
        smem=(0, 1, 2, 3),
    )

    sent = call(
        project,
        jax.ShapeDtypeStruct((8, 72, 128), bf16),
        [pltpu.VMEM((4, 32, 384), bf16)],
        where,
        sort,
        split,
        weights,
        *received,
        smem=(0,),
    )
    got = exchange(sent, ("y", "m0"))
    half = call(combine, jax.ShapeDtypeStruct((2, 72, 128), f32), [], got)
    got = lax.all_gather(half, "m1", axis=0, tiled=True)
    own = call(embed, jax.ShapeDtypeStruct((296, 128), bf16), [], got, codes)

    moves = []
    for s in range(512):
        o, rest = divmod(s, 32)
        moves.append((s, 32 * ((o - DELTA[rest % 4]) % 16) + rest))
    other = lax.ppermute(own, BATCH + MP, moves)
    sent = call(
        choose,
        jax.ShapeDtypeStruct((8, 296, 128), bf16),
        [pltpu.VMEM((2, 296, 128), bf16)],
        where,
        own,
        other,
        smem=(0,),
    )
    got = exchange(sent, Z)
    sent = call(
        score,
        jax.ShapeDtypeStruct((4, 72, 128), bf16),
        [],
        where,
        scalars,
        pairs,
        own,
        got,
        smem=(0,),
    )
    got = exchange(sent, MP)
    return call(
        finish,
        (jax.ShapeDtypeStruct((16, 288), f32), jax.ShapeDtypeStruct((4, 1152), f32)),
        [],
        got,
    )


def solution(mesh):
    finer = Mesh(mesh.devices.reshape(2, 2, 4, 2, 2, 2, 2, 2), BATCH + MP)
    in_specs = (P(BATCH, None), P(BATCH, None), P(BATCH, MP), P(BATCH, MP), P(BATCH), P(), P())
    out_specs = (P(BATCH, MP), P(BATCH + MP, None))

    return jax.shard_map(local, mesh=finer, in_specs=in_specs, out_specs=out_specs, check_vma=False)
```

```python
import jax
import jax.numpy as jnp
from jax import lax
from jax.experimental import pallas as pl
from jax.experimental.pallas import tpu as pltpu
from jax.sharding import Mesh
from jax.sharding import PartitionSpec as P


X = ("x1", "x0")
Z = ("z2", "z1", "z0")
BATCH = X + ("y",) + Z
SPREAD = ("z2", "z1", "z0", "x1", "x0")
Z_ORDER = ("z1", "z0", "z2")
MP = ("m0", "m1")
bf16 = jnp.bfloat16
f32 = jnp.float32
epsilon = 1e-06
DELTA = (-1, -2, 1, 2)


def place_in(order, **values):
    place = 0
    for axis in order:
        place = 2 * place + ((values[axis[0]] >> int(axis[1])) & 1)
    return place


def call(body, out_shape, scratch, *args, smem=(), hbm=(), out=pltpu.VMEM, vmem=16):
    spaces = [
        pltpu.SMEM if k in smem else pltpu.HBM if k in hbm else pltpu.VMEM for k in range(len(args))
    ]
    specs = [pl.BlockSpec(memory_space=space) for space in spaces]
    outs = jax.tree.map(lambda _: pl.BlockSpec(memory_space=out), out_shape)
    return pl.pallas_call(
        body, out_shape=out_shape, in_specs=specs, out_specs=outs, scratch_shapes=scratch,
        compiler_params=pltpu.CompilerParams(vmem_limit_bytes=vmem << 20),
    )(*args)


def pack(
    w_img_ref, w_txt_ref, img_ref, txt_ref, out_ref, c0_ref, c1_ref, c2_ref, c3_ref,
    w_img, w_txt, img, txt, rows, feats, in_sems, out_sems,
):
    moves = ((w_img_ref, w_img), (w_txt_ref, w_txt), (img_ref, img), (txt_ref, txt))
    reads = [pltpu.make_async_copy(a, b, in_sems.at[k]) for k, (a, b) in enumerate(moves)]
    for copy in reads:
        copy.start()
    for copy in reads[:2]:
        copy.wait()
    both = jnp.concatenate([w_img[...].astype(f32), w_txt[...].astype(f32)], axis=0)
    tail = jnp.concatenate([both[6 * g : 6 * g + 6, 256:288] for g in range(4)], axis=1)
    block = [both[:, 0:128], both[:, 128:256], tail, jnp.zeros((2, 128), f32)]
    block = jnp.concatenate(block, axis=0).astype(bf16)
    for k in range(8):
        rows[k] = block
    writes = [
        pltpu.make_async_copy(rows, out_ref.at[8 * k : 8 * k + 8], out_sems.at[k])
        for k in range(4)
    ]
    for copy in writes:
        copy.start()
    for copy in reads[2:]:
        copy.wait()
    for y in range(4):
        for which, feat in enumerate((img, txt)):
            for k in range(4):
                at = 384 * k + 96 * y
                feats[y, 16 * which : 16 * which + 16, 96 * k : 96 * k + 96] = feat[
                    :, at : at + 96
                ]
    here = lax.axis_index("y")
    more = [
        pltpu.make_async_copy(feats.at[(here + k) & 3], ref, out_sems.at[4 + k])
        for k, ref in enumerate((c0_ref, c1_ref, c2_ref, c3_ref))
    ]
    for copy in more:
        copy.start()
    for copy in writes + more:
        copy.wait()


def setup(
    where_ref, pair_ref, scale_ref, bias_ref, sort_ref, split_ref, pairs_ref, codes_ref, scalars_ref
):
    r = lax.broadcasted_iota(jnp.int32, (384, 384), 0)
    c = lax.broadcasted_iota(jnp.int32, (384, 384), 1)
    second = r >= 192
    k = jnp.where(second, r - 192, r)
    source = k + 12 * ((k * 171) >> 11) + jnp.where(second, 12, 0)
    sort_ref[...] = jnp.where(c == source, 1.0, 0.0).astype(bf16)
    k = lax.broadcasted_iota(jnp.int32, (192, 128), 0)
    c = lax.broadcasted_iota(jnp.int32, (192, 128), 1)
    group = (k * 171) >> 11
    inner = k - 12 * group
    low = (inner < 6) & (c == 8 * group + inner)
    high = (inner >= 6) & (c == 8 * group + inner - 6)
    split_ref[0:192, :] = jnp.where(low, 1.0, 0.0).astype(bf16)
    split_ref[192:384, :] = jnp.where(high, 1.0, 0.0).astype(bf16)
    row = lax.broadcasted_iota(jnp.int32, (16, 128), 0)
    lane = lax.broadcasted_iota(jnp.int32, (8, 128), 1)
    down = jnp.zeros((16, 128), jnp.int32)
    across = jnp.zeros((8, 128), jnp.int32)
    for k in range(16):
        down = jnp.where(row == k, pair_ref[k], down)
        across = jnp.where(lane == 16 * where_ref[1] + k, pair_ref[k], across)
    pairs_ref[...] = down
    row = lax.broadcasted_iota(jnp.int32, (8, 128), 0)
    codes_ref[...] = jnp.where(row == 0, across >> 6, across & 63).astype(f32)
    scalars_ref[0:8, :] = jnp.exp(jnp.full((8, 128), scale_ref[0], f32))
    scalars_ref[8:16, :] = jnp.full((8, 128), bias_ref[0], f32)


def project(
    where_ref, sort_ref, split_ref, w_ref, r0_ref, r1_ref, r2_ref, r3_ref, out_ref, feat_ref
):
    sort = sort_ref[...]
    low = split_ref[0:192, :]
    high = split_ref[192:384, :]
    weights = [[], []]
    for half in range(2):
        places = [
            place_in(SPREAD, x=q >> 3, z=q & 7) for q in range(16 * half, 16 * half + 16)
        ]
        some = jnp.stack([w_ref[place] for place in places], axis=0)
        main = jnp.concatenate(
            [some[:, 0:24].reshape(384, 128), some[:, 24:48].reshape(384, 128)], axis=1
        )
        tail = some[:, 48:56].reshape(128, 128)
        main = jnp.dot(sort, main, preferred_element_type=f32).astype(bf16)
        low_tail = jnp.dot(low, tail, preferred_element_type=f32)
        high_tail = jnp.dot(high, tail, preferred_element_type=f32)
        for which in range(2):
            at = 64 * which
            tail = low_tail[:, at : at + 32] + high_tail[:, at + 32 : at + 64]
            tail = tail.astype(bf16)
            weights[which].append(
                jnp.concatenate([main[192 * which : 192 * which + 192]] + [tail] * 4, axis=1)
            )
    y = where_ref[3]
    for k, ref in enumerate((r0_ref, r1_ref, r2_ref, r3_ref)):
        feat_ref[(y - k) & 3] = ref[...]
    parts = []
    for which in range(2):
        rows = jnp.concatenate(
            [feat_ref[s, 16 * which : 16 * which + 16, :] for s in range(4)], axis=0
        )
        part = jnp.dot(rows[:, 0:192], weights[which][0], preferred_element_type=f32)
        parts.append(
            part + jnp.dot(rows[:, 192:384], weights[which][1], preferred_element_type=f32)
        )
    for y in range(4):
        rows = jnp.concatenate([part[16 * y : 16 * y + 16] for part in parts], axis=0)
        tail = jnp.concatenate(
            [rows[8 * g : 8 * g + 8, 256 + 32 * g : 288 + 32 * g] for g in range(4)], axis=1
        )
        block = jnp.concatenate([rows[:, 0:128], rows[:, 128:256], tail], axis=0).astype(bf16)
        for m in range(2):
            out_ref[2 * y + m] = block


def combine(got_ref, out_ref):
    for m in range(2):
        pieces = [got_ref[2 * y + m].astype(f32) for y in range(4)]
        pre = pieces[0] + pieces[1] + pieces[2] + pieces[3]
        out_ref[m] = pre


def embed(got_ref, codes_ref, own_ref):
    total = jnp.zeros((32, 1), f32)
    tiles = []
    tails = []
    for col in range(4):
        pre = got_ref[2 * (col % 2) + col // 2]
        tiles += [pre[0:32], pre[32:64]]
        last = pre[64:72]
        tails.append(
            jnp.concatenate([last[:, 32 * g : 32 * g + 32] for g in range(4)], axis=0)
        )
    tiles.append(jnp.concatenate(tails, axis=1))
    for pre in tiles:
        total = total + jnp.sum(pre * pre, axis=1, keepdims=True)
    norm = lax.rsqrt(total + epsilon)
    for t, pre in enumerate(tiles):
        own_ref[32 * t : 32 * t + 32, :] = (pre * norm).astype(bf16)
    own_ref[288:296, :] = codes_ref[...].astype(bf16)


def choose(where_ref, own_ref, other_ref, out_ref, two_ref):
    z = where_ref[1]
    m = where_ref[2]
    two_ref[0] = own_ref[...]
    two_ref[1] = other_ref[...]
    near = (m == 0) | (m == 2)
    for to in range(8):
        other_img = near | ((m == 1) & (z >= to)) | ((m == 3) & (z < to))
        other_txt = near | ((m == 1) & (z > to)) | ((m == 3) & (z <= to))
        img = jnp.where(other_img, 1, 0)
        txt = jnp.where(other_txt, 1, 0)
        at = place_in(Z_ORDER, z=to)
        for t in range(9):
            out_ref[at, 32 * t : 32 * t + 16, :] = two_ref[img, 32 * t : 32 * t + 16, :]
            out_ref[at, 32 * t + 16 : 32 * t + 32, :] = two_ref[
                txt, 32 * t + 16 : 32 * t + 32, :
            ]
        out_ref[at, 288:296, :] = two_ref[img, 288:296, :]


def score(where_ref, scalars_ref, pair_ref, own_ref, got_ref, out_ref):
    octet = where_ref[0]
    z = where_ref[1]
    m = where_ref[2]
    scale = scalars_ref[0:1, :]
    scale_one = scale[:, 0:1]
    offset = scalars_ref[8:9, :]

    order = [place_in(Z_ORDER, z=k) for k in range(8)]

    def window(at):
        return jnp.concatenate(
            [
                jnp.concatenate(
                    [got_ref[k, 32 * t + at : 32 * t + at + 16, :] for k in order], axis=0
                )
                for t in range(9)
            ],
            axis=1,
        )

    def mine(at):
        return jnp.concatenate(
            [own_ref[32 * t + at : 32 * t + at + 16, :] for t in range(9)], axis=1
        )

    imgs = window(0)
    txts = window(16)
    codes = got_ref[0, 288:296, :].astype(f32)
    for k in range(1, 8):
        codes = codes + got_ref[k, 288:296, :].astype(f32)
    pair_window = codes[0:1] * 64.0 + codes[1:2]
    lane = lax.broadcasted_iota(jnp.int32, (16, 128), 1)
    row = lax.broadcasted_iota(jnp.int32, (16, 128), 0)
    there = lane >> 4
    behind = jnp.where(there > z, -2, 0)
    ahead = jnp.where(there > z, 0, 2)
    delta = jnp.where(m == 1, behind, jnp.where(m == 3, ahead, m - 1))
    block = (8 * (octet + delta) + there) & 127
    text_index = block * 16 + (lane & 15)
    match_img = pair_ref[...] == text_index
    own_text = (octet * 8 + z) * 16 + row
    match_txt = pair_window == own_text.astype(f32)

    def grads(own, window, match):
        scores = lax.dot_general(own, window, (((1,), (1,)), ((), ())), preferred_element_type=f32)
        logits = scale * scores + offset
        label = jnp.where(match, 1.0, -1.0)
        coef = (-label / (1.0 + jnp.exp(label * logits))).astype(bf16)
        return scale_one * jnp.dot(coef, window, preferred_element_type=f32)

    image_part = grads(mine(0), txts, match_img)
    text_part = grads(mine(16), imgs, match_txt)
    for to in range(4):
        rows = text_part[4 * to : 4 * to + 4]
        at = 1024 + 32 * to
        pieces = [
            image_part[:, 256 * to : 256 * to + 128],
            image_part[:, 256 * to + 128 : 256 * to + 256],
        ]
        pieces += [rows[:, 128 * t : 128 * t + 128] for t in range(9)]
        pieces.append(
            jnp.concatenate(
                [image_part[4 * g : 4 * g + 4, at : at + 32] for g in range(4)], axis=1
            )
        )
        out_ref[to] = jnp.concatenate(pieces, axis=0).astype(bf16)


def finish(got_ref, image_ref, text_ref):
    total = got_ref[0].astype(f32)
    for k in range(1, 4):
        total = total + got_ref[k].astype(f32)
    image_ref[:, 0:128] = total[0:16]
    image_ref[:, 128:256] = total[16:32]
    image_ref[:, 256:288] = jnp.concatenate(
        [total[68:72, 32 * g : 32 * g + 32] for g in range(4)], axis=0
    )
    pieces = []
    for c in range(4):
        pieces += [total[32 + 8 * c : 36 + 8 * c], total[36 + 8 * c : 40 + 8 * c]]
        pieces.append(total[64:68, 32 * c : 32 * c + 32])
    text_ref[...] = jnp.concatenate(pieces, axis=1)


def exchange(value, axes):
    return lax.all_to_all(value, axes, split_axis=0, concat_axis=0, tiled=True)


def local(img_feat, txt_feat, w_img, w_txt, pair_index, log_scale, bias):
    x, y, z = (lax.axis_index(a) for a in (X, "y", Z))
    m = lax.axis_index(MP)
    octet = 4 * x + y
    where = jnp.stack([octet, z, m, y]).astype(jnp.int32)

    sent, *chosen = call(
        pack,
        (jax.ShapeDtypeStruct((32, 56, 128), bf16),)
        + (jax.ShapeDtypeStruct((32, 384), bf16),) * 4,
        [pltpu.VMEM((12, 288), bf16)] * 2
        + [pltpu.VMEM((16, 1536), bf16)] * 2
        + [pltpu.VMEM((8, 56, 128), bf16), pltpu.VMEM((4, 32, 384), bf16)]
        + [pltpu.SemaphoreType.DMA((4,)), pltpu.SemaphoreType.DMA((8,))],
        w_img,
        w_txt,
        img_feat,
        txt_feat,
        hbm=(0, 1, 2, 3),
        out=pltpu.HBM,
        vmem=60,
    )
    weights = exchange(sent, SPREAD)

    received = [chosen[0]]
    for k in range(1, 4):
        received.append(
            lax.ppermute(chosen[k], "y", [(s, (s + k) % 4) for s in range(4)])
        )

    sort, split, pairs, codes, scalars = call(
        setup,
        (
            jax.ShapeDtypeStruct((384, 384), bf16),
            jax.ShapeDtypeStruct((384, 128), bf16),
            jax.ShapeDtypeStruct((16, 128), jnp.int32),
            jax.ShapeDtypeStruct((8, 128), f32),
            jax.ShapeDtypeStruct((16, 128), f32),
        ),
        [],
        where,
        pair_index,
        log_scale,
        bias,
        smem=(0, 1, 2, 3),
    )

    sent = call(
        project,
        jax.ShapeDtypeStruct((8, 72, 128), bf16),
        [pltpu.VMEM((4, 32, 384), bf16)],
        where,
        sort,
        split,
        weights,
        *received,
        smem=(0,),
    )
    got = exchange(sent, ("y", "m0"))
    half = call(combine, jax.ShapeDtypeStruct((2, 72, 128), f32), [], got)
    got = lax.all_gather(half, "m1", axis=0, tiled=True)
    own = call(embed, jax.ShapeDtypeStruct((296, 128), bf16), [], got, codes)

    moves = []
    for s in range(512):
        o, rest = divmod(s, 32)
        moves.append((s, 32 * ((o - DELTA[rest % 4]) % 16) + rest))
    other = lax.ppermute(own, BATCH + MP, moves)
    sent = call(
        choose,
        jax.ShapeDtypeStruct((8, 296, 128), bf16),
        [pltpu.VMEM((2, 296, 128), bf16)],
        where,
        own,
        other,
        smem=(0,),
    )
    got = exchange(sent, Z_ORDER)
    sent = call(
        score,
        jax.ShapeDtypeStruct((4, 72, 128), bf16),
        [],
        where,
        scalars,
        pairs,
        own,
        got,
        smem=(0,),
    )
    got = exchange(sent, MP)
    return call(
        finish,
        (jax.ShapeDtypeStruct((16, 288), f32), jax.ShapeDtypeStruct((4, 1152), f32)),
        [],
        got,
    )


def solution(mesh):
    finer = Mesh(mesh.devices.reshape(2, 2, 4, 2, 2, 2, 2, 2), BATCH + MP)
    in_specs = (P(BATCH, None), P(BATCH, None), P(BATCH, MP), P(BATCH, MP), P(BATCH), P(), P())
    out_specs = (P(BATCH, MP), P(BATCH + MP, None))

    return jax.shard_map(local, mesh=finer, in_specs=in_specs, out_specs=out_specs, check_vma=False)
```

```python
import jax
import jax.numpy as jnp
from jax import lax
from jax.experimental import pallas as pl
from jax.experimental.pallas import tpu as pltpu
from jax.sharding import Mesh
from jax.sharding import PartitionSpec as P


X = ("x1", "x0")
Z = ("z2", "z1", "z0")
BATCH = X + ("y",) + Z
SPREAD = ("z2", "z1", "z0", "x1", "x0")
Z_ORDER = ("z1", "z0", "z2")
MP = ("m0", "m1")
bf16 = jnp.bfloat16
f32 = jnp.float32
epsilon = 1e-06
DELTA = (-1, -2, 1, 2)


def place_in(order, **values):
    place = 0
    for axis in order:
        place = 2 * place + ((values[axis[0]] >> int(axis[1])) & 1)
    return place


def call(body, out_shape, scratch, *args, smem=(), hbm=(), out=pltpu.VMEM, vmem=16):
    spaces = [
        pltpu.SMEM if k in smem else pltpu.HBM if k in hbm else pltpu.VMEM for k in range(len(args))
    ]
    specs = [pl.BlockSpec(memory_space=space) for space in spaces]
    outs = jax.tree.map(lambda _: pl.BlockSpec(memory_space=out), out_shape)
    return pl.pallas_call(
        body, out_shape=out_shape, in_specs=specs, out_specs=outs, scratch_shapes=scratch,
        compiler_params=pltpu.CompilerParams(vmem_limit_bytes=vmem << 20),
    )(*args)


def pack(
    w_img_ref, w_txt_ref, img_ref, txt_ref, out_ref, c0_ref, c1_ref, c2_ref, c3_ref,
    w_img, w_txt, img, txt, rows, feats, in_sems, out_sems,
):
    moves = ((w_img_ref, w_img), (w_txt_ref, w_txt), (img_ref, img), (txt_ref, txt))
    reads = [pltpu.make_async_copy(a, b, in_sems.at[k]) for k, (a, b) in enumerate(moves)]
    for copy in reads:
        copy.start()
    for copy in reads[:2]:
        copy.wait()
    both = jnp.concatenate([w_img[...].astype(f32), w_txt[...].astype(f32)], axis=0)
    tail = jnp.concatenate([both[6 * g : 6 * g + 6, 256:288] for g in range(4)], axis=1)
    block = [both[:, 0:128], both[:, 128:256], tail, jnp.zeros((2, 128), f32)]
    block = jnp.concatenate(block, axis=0).astype(bf16)
    for k in range(8):
        rows[k] = block
    writes = [
        pltpu.make_async_copy(rows, out_ref.at[8 * k : 8 * k + 8], out_sems.at[k])
        for k in range(4)
    ]
    for copy in writes:
        copy.start()
    for copy in reads[2:]:
        copy.wait()
    for y in range(4):
        for which, feat in enumerate((img, txt)):
            for k in range(4):
                at = 384 * k + 96 * y
                feats[y, 16 * which : 16 * which + 16, 96 * k : 96 * k + 96] = feat[
                    :, at : at + 96
                ]
    here = lax.axis_index("y")
    more = [
        pltpu.make_async_copy(feats.at[(here + k) & 3], ref, out_sems.at[4 + k])
        for k, ref in enumerate((c0_ref, c1_ref, c2_ref, c3_ref))
    ]
    for copy in more:
        copy.start()
    for copy in writes + more:
        copy.wait()


def setup(
    where_ref, pair_ref, scale_ref, bias_ref, sort_ref, split_ref, pairs_ref, codes_ref, scalars_ref
):
    r = lax.broadcasted_iota(jnp.int32, (384, 384), 0)
    c = lax.broadcasted_iota(jnp.int32, (384, 384), 1)
    second = r >= 192
    k = jnp.where(second, r - 192, r)
    source = k + 12 * ((k * 171) >> 11) + jnp.where(second, 12, 0)
    sort_ref[...] = jnp.where(c == source, 1.0, 0.0).astype(bf16)
    k = lax.broadcasted_iota(jnp.int32, (192, 128), 0)
    c = lax.broadcasted_iota(jnp.int32, (192, 128), 1)
    group = (k * 171) >> 11
    inner = k - 12 * group
    low = (inner < 6) & (c == 8 * group + inner)
    high = (inner >= 6) & (c == 8 * group + inner - 6)
    split_ref[0:192, :] = jnp.where(low, 1.0, 0.0).astype(bf16)
    split_ref[192:384, :] = jnp.where(high, 1.0, 0.0).astype(bf16)
    row = lax.broadcasted_iota(jnp.int32, (16, 128), 0)
    lane = lax.broadcasted_iota(jnp.int32, (8, 128), 1)
    down = jnp.zeros((16, 128), jnp.int32)
    across = jnp.zeros((8, 128), jnp.int32)
    for k in range(16):
        down = jnp.where(row == k, pair_ref[k], down)
        across = jnp.where(lane == 16 * where_ref[1] + k, pair_ref[k], across)
    pairs_ref[...] = down
    row = lax.broadcasted_iota(jnp.int32, (8, 128), 0)
    codes_ref[...] = jnp.where(row == 0, across >> 6, across & 63).astype(f32)
    scalars_ref[0:8, :] = jnp.exp(jnp.full((8, 128), scale_ref[0], f32))
    scalars_ref[8:16, :] = jnp.full((8, 128), bias_ref[0], f32)


def project(
    where_ref, sort_ref, split_ref, w_ref, r0_ref, r1_ref, r2_ref, r3_ref, out_ref, feat_ref
):
    sort = sort_ref[...]
    low = split_ref[0:192, :]
    high = split_ref[192:384, :]
    weights = [[], []]
    for half in range(2):
        places = [
            place_in(SPREAD, x=q >> 3, z=q & 7) for q in range(16 * half, 16 * half + 16)
        ]
        some = jnp.stack([w_ref[place] for place in places], axis=0)
        main = jnp.concatenate(
            [some[:, 0:24].reshape(384, 128), some[:, 24:48].reshape(384, 128)], axis=1
        )
        tail = some[:, 48:56].reshape(128, 128)
        main = jnp.dot(sort, main, preferred_element_type=f32).astype(bf16)
        low_tail = jnp.dot(low, tail, preferred_element_type=f32)
        high_tail = jnp.dot(high, tail, preferred_element_type=f32)
        for which in range(2):
            at = 64 * which
            tail = low_tail[:, at : at + 32] + high_tail[:, at + 32 : at + 64]
            tail = tail.astype(bf16)
            weights[which].append(
                jnp.concatenate([main[192 * which : 192 * which + 192]] + [tail] * 4, axis=1)
            )
    y = where_ref[3]
    for k, ref in enumerate((r0_ref, r1_ref, r2_ref, r3_ref)):
        feat_ref[(y - k) & 3] = ref[...]
    parts = []
    for which in range(2):
        rows = jnp.concatenate(
            [feat_ref[s, 16 * which : 16 * which + 16, :] for s in range(4)], axis=0
        )
        part = jnp.dot(rows[:, 0:192], weights[which][0], preferred_element_type=f32)
        parts.append(
            part + jnp.dot(rows[:, 192:384], weights[which][1], preferred_element_type=f32)
        )
    for y in range(4):
        rows = jnp.concatenate([part[16 * y : 16 * y + 16] for part in parts], axis=0)
        tail = jnp.concatenate(
            [rows[8 * g : 8 * g + 8, 256 + 32 * g : 288 + 32 * g] for g in range(4)], axis=1
        )
        block = jnp.concatenate([rows[:, 0:128], rows[:, 128:256], tail], axis=0).astype(bf16)
        for m in range(2):
            out_ref[2 * y + m] = block


def combine(got_ref, out_ref):
    for m in range(2):
        pieces = [got_ref[2 * y + m].astype(f32) for y in range(4)]
        pre = pieces[0] + pieces[1] + pieces[2] + pieces[3]
        out_ref[m] = pre


def embed(got_ref, codes_ref, own_ref):
    total = jnp.zeros((32, 1), f32)
    tiles = []
    tails = []
    for col in range(4):
        pre = got_ref[2 * (col % 2) + col // 2]
        tiles += [pre[0:32], pre[32:64]]
        last = pre[64:72]
        tails.append(
            jnp.concatenate([last[:, 32 * g : 32 * g + 32] for g in range(4)], axis=0)
        )
    tiles.append(jnp.concatenate(tails, axis=1))
    for pre in tiles:
        total = total + jnp.sum(pre * pre, axis=1, keepdims=True)
    norm = lax.rsqrt(total + epsilon)
    for t, pre in enumerate(tiles):
        own_ref[32 * t : 32 * t + 32, :] = (pre * norm).astype(bf16)
    own_ref[288:296, :] = codes_ref[...].astype(bf16)


def choose(where_ref, own_ref, other_ref, out_ref, two_ref):
    z = where_ref[1]
    m = where_ref[2]
    two_ref[0] = own_ref[...]
    two_ref[1] = other_ref[...]
    near = (m == 0) | (m == 2)
    for to in range(8):
        other_img = near | ((m == 1) & (z >= to)) | ((m == 3) & (z < to))
        other_txt = near | ((m == 1) & (z > to)) | ((m == 3) & (z <= to))
        img = jnp.where(other_img, 1, 0)
        txt = jnp.where(other_txt, 1, 0)
        at = place_in(Z_ORDER, z=to)
        for t in range(9):
            out_ref[at, 32 * t : 32 * t + 16, :] = two_ref[img, 32 * t : 32 * t + 16, :]
            out_ref[at, 32 * t + 16 : 32 * t + 32, :] = two_ref[
                txt, 32 * t + 16 : 32 * t + 32, :
            ]
        out_ref[at, 288:296, :] = two_ref[img, 288:296, :]


def score(where_ref, scalars_ref, pair_ref, own_ref, got_ref, out_ref):
    octet = where_ref[0]
    z = where_ref[1]
    m = where_ref[2]
    scale = scalars_ref[0:1, :]
    scale_one = scale[:, 0:1]
    offset = scalars_ref[8:9, :]

    order = [place_in(Z_ORDER, z=k) for k in range(8)]

    def window(at):
        return jnp.concatenate(
            [
                jnp.concatenate(
                    [got_ref[k, 32 * t + at : 32 * t + at + 16, :] for k in order], axis=0
                )
                for t in range(9)
            ],
            axis=1,
        )

    def mine(at):
        return jnp.concatenate(
            [own_ref[32 * t + at : 32 * t + at + 16, :] for t in range(9)], axis=1
        )

    imgs = window(0)
    txts = window(16)
    codes = got_ref[0, 288:296, :].astype(f32)
    for k in range(1, 8):
        codes = codes + got_ref[k, 288:296, :].astype(f32)
    pair_window = codes[0:1] * 64.0 + codes[1:2]
    lane = lax.broadcasted_iota(jnp.int32, (16, 128), 1)
    row = lax.broadcasted_iota(jnp.int32, (16, 128), 0)
    there = lane >> 4
    behind = jnp.where(there > z, -2, 0)
    ahead = jnp.where(there > z, 0, 2)
    delta = jnp.where(m == 1, behind, jnp.where(m == 3, ahead, m - 1))
    block = (8 * (octet + delta) + there) & 127
    text_index = block * 16 + (lane & 15)
    match_img = pair_ref[...] == text_index
    own_text = (octet * 8 + z) * 16 + row
    match_txt = pair_window == own_text.astype(f32)

    sides = ((mine(0), txts, match_img), (mine(16), imgs, match_txt))
    scores = [
        lax.dot_general(own, window, (((1,), (1,)), ((), ())), preferred_element_type=f32)
        for own, window, _ in sides
    ]
    coefs = []
    for score, (_, _, match) in zip(scores, sides):
        label = jnp.where(match, 1.0, -1.0)
        coefs.append((-label / (1.0 + jnp.exp(label * (scale * score + offset)))).astype(bf16))
    image_part, text_part = (
        scale_one * jnp.dot(coef, window, preferred_element_type=f32)
        for coef, (_, window, _) in zip(coefs, sides)
    )
    for to in range(4):
        rows = text_part[4 * to : 4 * to + 4]
        at = 1024 + 32 * to
        pieces = [
            image_part[:, 256 * to : 256 * to + 128],
            image_part[:, 256 * to + 128 : 256 * to + 256],
        ]
        pieces += [rows[:, 128 * t : 128 * t + 128] for t in range(9)]
        pieces.append(
            jnp.concatenate(
                [image_part[4 * g : 4 * g + 4, at : at + 32] for g in range(4)], axis=1
            )
        )
        out_ref[to] = jnp.concatenate(pieces, axis=0).astype(bf16)


def finish(got_ref, image_ref, text_ref):
    total = got_ref[0].astype(f32)
    for k in range(1, 4):
        total = total + got_ref[k].astype(f32)
    image_ref[:, 0:128] = total[0:16]
    image_ref[:, 128:256] = total[16:32]
    image_ref[:, 256:288] = jnp.concatenate(
        [total[68:72, 32 * g : 32 * g + 32] for g in range(4)], axis=0
    )
    pieces = []
    for c in range(4):
        pieces += [total[32 + 8 * c : 36 + 8 * c], total[36 + 8 * c : 40 + 8 * c]]
        pieces.append(total[64:68, 32 * c : 32 * c + 32])
    text_ref[...] = jnp.concatenate(pieces, axis=1)


def exchange(value, axes):
    return lax.all_to_all(value, axes, split_axis=0, concat_axis=0, tiled=True)


def local(img_feat, txt_feat, w_img, w_txt, pair_index, log_scale, bias):
    x, y, z = (lax.axis_index(a) for a in (X, "y", Z))
    m = lax.axis_index(MP)
    octet = 4 * x + y
    where = jnp.stack([octet, z, m, y]).astype(jnp.int32)

    sent, *chosen = call(
        pack,
        (jax.ShapeDtypeStruct((32, 56, 128), bf16),)
        + (jax.ShapeDtypeStruct((32, 384), bf16),) * 4,
        [pltpu.VMEM((12, 288), bf16)] * 2
        + [pltpu.VMEM((16, 1536), bf16)] * 2
        + [pltpu.VMEM((8, 56, 128), bf16), pltpu.VMEM((4, 32, 384), bf16)]
        + [pltpu.SemaphoreType.DMA((4,)), pltpu.SemaphoreType.DMA((8,))],
        w_img,
        w_txt,
        img_feat,
        txt_feat,
        hbm=(0, 1, 2, 3),
        out=pltpu.HBM,
        vmem=60,
    )
    weights = exchange(sent, SPREAD)

    received = [chosen[0]]
    for k in range(1, 4):
        received.append(
            lax.ppermute(chosen[k], "y", [(s, (s + k) % 4) for s in range(4)])
        )

    sort, split, pairs, codes, scalars = call(
        setup,
        (
            jax.ShapeDtypeStruct((384, 384), bf16),
            jax.ShapeDtypeStruct((384, 128), bf16),
            jax.ShapeDtypeStruct((16, 128), jnp.int32),
            jax.ShapeDtypeStruct((8, 128), f32),
            jax.ShapeDtypeStruct((16, 128), f32),
        ),
        [],
        where,
        pair_index,
        log_scale,
        bias,
        smem=(0, 1, 2, 3),
    )

    sent = call(
        project,
        jax.ShapeDtypeStruct((8, 72, 128), bf16),
        [pltpu.VMEM((4, 32, 384), bf16)],
        where,
        sort,
        split,
        weights,
        *received,
        smem=(0,),
    )
    got = exchange(sent, ("y", "m0"))
    half = call(combine, jax.ShapeDtypeStruct((2, 72, 128), f32), [], got)
    got = lax.all_gather(half, "m1", axis=0, tiled=True)
    own = call(embed, jax.ShapeDtypeStruct((296, 128), bf16), [], got, codes)

    moves = []
    for s in range(512):
        o, rest = divmod(s, 32)
        moves.append((s, 32 * ((o - DELTA[rest % 4]) % 16) + rest))
    other = lax.ppermute(own, BATCH + MP, moves)
    sent = call(
        choose,
        jax.ShapeDtypeStruct((8, 296, 128), bf16),
        [pltpu.VMEM((2, 296, 128), bf16)],
        where,
        own,
        other,
        smem=(0,),
    )
    got = exchange(sent, Z_ORDER)
    sent = call(
        score,
        jax.ShapeDtypeStruct((4, 72, 128), bf16),
        [],
        where,
        scalars,
        pairs,
        own,
        got,
        smem=(0,),
    )
    got = exchange(sent, MP)
    return call(
        finish,
        (jax.ShapeDtypeStruct((16, 288), f32), jax.ShapeDtypeStruct((4, 1152), f32)),
        [],
        got,
    )


def solution(mesh):
    finer = Mesh(mesh.devices.reshape(2, 2, 4, 2, 2, 2, 2, 2), BATCH + MP)
    in_specs = (P(BATCH, None), P(BATCH, None), P(BATCH, MP), P(BATCH, MP), P(BATCH), P(), P())
    out_specs = (P(BATCH, MP), P(BATCH + MP, None))

    return jax.shard_map(local, mesh=finer, in_specs=in_specs, out_specs=out_specs, check_vma=False)
```

```python
import jax
import jax.numpy as jnp
from jax import lax
from jax.experimental import pallas as pl
from jax.experimental.pallas import tpu as pltpu
from jax.sharding import Mesh
from jax.sharding import PartitionSpec as P


X = ("x1", "x0")
Z = ("z2", "z1", "z0")
BATCH = X + ("y",) + Z
SPREAD = ("z2", "z1", "z0", "x1", "x0")
Z_ORDER = ("z1", "z0", "z2")
MP = ("m0", "m1")
bf16 = jnp.bfloat16
f32 = jnp.float32
epsilon = 1e-06
DELTA = (-1, -2, 1, 2)


def place_in(order, **values):
    place = 0
    for axis in order:
        place = 2 * place + ((values[axis[0]] >> int(axis[1])) & 1)
    return place


def call(body, out_shape, scratch, *args, smem=(), hbm=(), out=pltpu.VMEM, vmem=16):
    spaces = [
        pltpu.SMEM if k in smem else pltpu.HBM if k in hbm else pltpu.VMEM for k in range(len(args))
    ]
    specs = [pl.BlockSpec(memory_space=space) for space in spaces]
    outs = jax.tree.map(lambda _: pl.BlockSpec(memory_space=out), out_shape)
    return pl.pallas_call(
        body, out_shape=out_shape, in_specs=specs, out_specs=outs, scratch_shapes=scratch,
        compiler_params=pltpu.CompilerParams(vmem_limit_bytes=vmem << 20),
    )(*args)


def pack(
    w_img_ref, w_txt_ref, img_ref, txt_ref, out_ref, c0_ref, c1_ref, c2_ref, c3_ref,
    w_img, w_txt, img, txt, rows, feats, in_sems, out_sems,
):
    moves = ((w_img_ref, w_img), (w_txt_ref, w_txt), (img_ref, img), (txt_ref, txt))
    reads = [pltpu.make_async_copy(a, b, in_sems.at[k]) for k, (a, b) in enumerate(moves)]
    for copy in reads:
        copy.start()
    for copy in reads[:2]:
        copy.wait()
    both = jnp.concatenate([w_img[...].astype(f32), w_txt[...].astype(f32)], axis=0)
    tail = jnp.concatenate([both[6 * g : 6 * g + 6, 256:288] for g in range(4)], axis=1)
    block = [both[:, 0:128], both[:, 128:256], tail, jnp.zeros((2, 128), f32)]
    block = jnp.concatenate(block, axis=0).astype(bf16)
    for k in range(8):
        rows[k] = block
    writes = [
        pltpu.make_async_copy(rows, out_ref.at[8 * k : 8 * k + 8], out_sems.at[k])
        for k in range(4)
    ]
    for copy in writes:
        copy.start()
    for copy in reads[2:]:
        copy.wait()
    for y in range(4):
        for which, feat in enumerate((img, txt)):
            for k in range(4):
                at = 384 * k + 96 * y
                feats[y, 16 * which : 16 * which + 16, 96 * k : 96 * k + 96] = feat[
                    :, at : at + 96
                ]
    here = lax.axis_index("y")
    more = [
        pltpu.make_async_copy(feats.at[(here + k) & 3], ref, out_sems.at[4 + k])
        for k, ref in enumerate((c0_ref, c1_ref, c2_ref, c3_ref))
    ]
    for copy in more:
        copy.start()
    for copy in writes + more:
        copy.wait()


def setup(
    where_ref, pair_ref, scale_ref, bias_ref, sort_ref, split_ref, pairs_ref, codes_ref, scalars_ref
):
    r = lax.broadcasted_iota(jnp.int32, (384, 384), 0)
    c = lax.broadcasted_iota(jnp.int32, (384, 384), 1)
    second = r >= 192
    k = jnp.where(second, r - 192, r)
    source = k + 12 * ((k * 171) >> 11) + jnp.where(second, 12, 0)
    sort_ref[...] = jnp.where(c == source, 1.0, 0.0).astype(bf16)
    k = lax.broadcasted_iota(jnp.int32, (192, 128), 0)
    c = lax.broadcasted_iota(jnp.int32, (192, 128), 1)
    group = (k * 171) >> 11
    inner = k - 12 * group
    low = (inner < 6) & (c == 8 * group + inner)
    high = (inner >= 6) & (c == 8 * group + inner - 6)
    split_ref[0:192, :] = jnp.where(low, 1.0, 0.0).astype(bf16)
    split_ref[192:384, :] = jnp.where(high, 1.0, 0.0).astype(bf16)
    row = lax.broadcasted_iota(jnp.int32, (16, 128), 0)
    lane = lax.broadcasted_iota(jnp.int32, (8, 128), 1)
    down = jnp.zeros((16, 128), jnp.int32)
    across = jnp.zeros((8, 128), jnp.int32)
    for k in range(16):
        down = jnp.where(row == k, pair_ref[k], down)
        across = jnp.where(lane == 16 * where_ref[1] + k, pair_ref[k], across)
    pairs_ref[...] = down
    row = lax.broadcasted_iota(jnp.int32, (8, 128), 0)
    codes_ref[...] = jnp.where(row == 0, across >> 6, across & 63).astype(f32)
    scalars_ref[0:8, :] = jnp.exp(jnp.full((8, 128), scale_ref[0], f32))
    scalars_ref[8:16, :] = jnp.full((8, 128), bias_ref[0], f32)


def project(
    where_ref, sort_ref, split_ref, w_ref, r0_ref, r1_ref, r2_ref, r3_ref, out_ref, feat_ref
):
    sort = sort_ref[...]
    low = split_ref[0:192, :]
    high = split_ref[192:384, :]
    mains = []
    tails = []
    for half in range(2):
        places = [
            place_in(SPREAD, x=q >> 3, z=q & 7) for q in range(16 * half, 16 * half + 16)
        ]
        some = jnp.stack([w_ref[place] for place in places], axis=0)
        mains.append(
            jnp.concatenate(
                [some[:, 0:24].reshape(384, 128), some[:, 24:48].reshape(384, 128)], axis=1
            )
        )
        tails.append(some[:, 48:56].reshape(128, 128))
    mains = [jnp.dot(sort, main, preferred_element_type=f32) for main in mains]
    lows = [jnp.dot(low, tail, preferred_element_type=f32) for tail in tails]
    highs = [jnp.dot(high, tail, preferred_element_type=f32) for tail in tails]
    weights = [[], []]
    for half in range(2):
        main = mains[half].astype(bf16)
        for which in range(2):
            at = 64 * which
            tail = lows[half][:, at : at + 32] + highs[half][:, at + 32 : at + 64]
            tail = tail.astype(bf16)
            weights[which].append(
                jnp.concatenate([main[192 * which : 192 * which + 192]] + [tail] * 4, axis=1)
            )
    y = where_ref[3]
    for k, ref in enumerate((r0_ref, r1_ref, r2_ref, r3_ref)):
        feat_ref[(y - k) & 3] = ref[...]
    parts = []
    for which in range(2):
        rows = jnp.concatenate(
            [feat_ref[s, 16 * which : 16 * which + 16, :] for s in range(4)], axis=0
        )
        part = jnp.dot(rows[:, 0:192], weights[which][0], preferred_element_type=f32)
        parts.append(
            part + jnp.dot(rows[:, 192:384], weights[which][1], preferred_element_type=f32)
        )
    for y in range(4):
        rows = jnp.concatenate([part[16 * y : 16 * y + 16] for part in parts], axis=0)
        tail = jnp.concatenate(
            [rows[8 * g : 8 * g + 8, 256 + 32 * g : 288 + 32 * g] for g in range(4)], axis=1
        )
        block = jnp.concatenate([rows[:, 0:128], rows[:, 128:256], tail], axis=0).astype(bf16)
        for m in range(2):
            out_ref[2 * y + m] = block


def combine(got_ref, out_ref):
    for m in range(2):
        pieces = [got_ref[2 * y + m].astype(f32) for y in range(4)]
        pre = pieces[0] + pieces[1] + pieces[2] + pieces[3]
        out_ref[m] = pre


def embed(got_ref, codes_ref, own_ref):
    total = jnp.zeros((32, 1), f32)
    tiles = []
    tails = []
    for col in range(4):
        pre = got_ref[2 * (col % 2) + col // 2]
        tiles += [pre[0:32], pre[32:64]]
        last = pre[64:72]
        tails.append(
            jnp.concatenate([last[:, 32 * g : 32 * g + 32] for g in range(4)], axis=0)
        )
    tiles.append(jnp.concatenate(tails, axis=1))
    for pre in tiles:
        total = total + jnp.sum(pre * pre, axis=1, keepdims=True)
    norm = lax.rsqrt(total + epsilon)
    for t, pre in enumerate(tiles):
        own_ref[32 * t : 32 * t + 32, :] = (pre * norm).astype(bf16)
    own_ref[288:296, :] = codes_ref[...].astype(bf16)


def choose(where_ref, own_ref, other_ref, out_ref, two_ref):
    z = where_ref[1]
    m = where_ref[2]
    two_ref[0] = own_ref[...]
    two_ref[1] = other_ref[...]
    near = (m == 0) | (m == 2)
    for to in range(8):
        other_img = near | ((m == 1) & (z >= to)) | ((m == 3) & (z < to))
        other_txt = near | ((m == 1) & (z > to)) | ((m == 3) & (z <= to))
        img = jnp.where(other_img, 1, 0)
        txt = jnp.where(other_txt, 1, 0)
        at = place_in(Z_ORDER, z=to)
        for t in range(9):
            out_ref[at, 32 * t : 32 * t + 16, :] = two_ref[img, 32 * t : 32 * t + 16, :]
            out_ref[at, 32 * t + 16 : 32 * t + 32, :] = two_ref[
                txt, 32 * t + 16 : 32 * t + 32, :
            ]
        out_ref[at, 288:296, :] = two_ref[img, 288:296, :]


def score(where_ref, scalars_ref, pair_ref, own_ref, got_ref, out_ref):
    octet = where_ref[0]
    z = where_ref[1]
    m = where_ref[2]
    scale = scalars_ref[0:1, :]
    scale_one = scale[:, 0:1]
    offset = scalars_ref[8:9, :]

    order = [place_in(Z_ORDER, z=k) for k in range(8)]

    def window(at):
        return jnp.concatenate(
            [
                jnp.concatenate(
                    [got_ref[k, 32 * t + at : 32 * t + at + 16, :] for k in order], axis=0
                )
                for t in range(9)
            ],
            axis=1,
        )

    def mine(at):
        return jnp.concatenate(
            [own_ref[32 * t + at : 32 * t + at + 16, :] for t in range(9)], axis=1
        )

    imgs = window(0)
    txts = window(16)
    codes = got_ref[0, 288:296, :].astype(f32)
    for k in range(1, 8):
        codes = codes + got_ref[k, 288:296, :].astype(f32)
    pair_window = codes[0:1] * 64.0 + codes[1:2]
    lane = lax.broadcasted_iota(jnp.int32, (16, 128), 1)
    row = lax.broadcasted_iota(jnp.int32, (16, 128), 0)
    there = lane >> 4
    behind = jnp.where(there > z, -2, 0)
    ahead = jnp.where(there > z, 0, 2)
    delta = jnp.where(m == 1, behind, jnp.where(m == 3, ahead, m - 1))
    block = (8 * (octet + delta) + there) & 127
    text_index = block * 16 + (lane & 15)
    match_img = pair_ref[...] == text_index
    own_text = (octet * 8 + z) * 16 + row
    match_txt = pair_window == own_text.astype(f32)

    sides = ((mine(0), txts, match_img), (mine(16), imgs, match_txt))
    scores = [
        lax.dot_general(own, window, (((1,), (1,)), ((), ())), preferred_element_type=f32)
        for own, window, _ in sides
    ]
    coefs = []
    for score, (_, _, match) in zip(scores, sides):
        label = jnp.where(match, 1.0, -1.0)
        coefs.append((-label / (1.0 + jnp.exp(label * (scale * score + offset)))).astype(bf16))
    image_part, text_part = (
        scale_one * jnp.dot(coef, window, preferred_element_type=f32)
        for coef, (_, window, _) in zip(coefs, sides)
    )
    for to in range(4):
        rows = text_part[4 * to : 4 * to + 4]
        at = 1024 + 32 * to
        pieces = [
            image_part[:, 256 * to : 256 * to + 128],
            image_part[:, 256 * to + 128 : 256 * to + 256],
        ]
        pieces += [rows[:, 128 * t : 128 * t + 128] for t in range(9)]
        pieces.append(
            jnp.concatenate(
                [image_part[4 * g : 4 * g + 4, at : at + 32] for g in range(4)], axis=1
            )
        )
        out_ref[to] = jnp.concatenate(pieces, axis=0).astype(bf16)


def finish(got_ref, image_ref, text_ref):
    total = got_ref[0].astype(f32)
    for k in range(1, 4):
        total = total + got_ref[k].astype(f32)
    image_ref[:, 0:128] = total[0:16]
    image_ref[:, 128:256] = total[16:32]
    image_ref[:, 256:288] = jnp.concatenate(
        [total[68:72, 32 * g : 32 * g + 32] for g in range(4)], axis=0
    )
    pieces = []
    for c in range(4):
        pieces += [total[32 + 8 * c : 36 + 8 * c], total[36 + 8 * c : 40 + 8 * c]]
        pieces.append(total[64:68, 32 * c : 32 * c + 32])
    text_ref[...] = jnp.concatenate(pieces, axis=1)


def exchange(value, axes):
    return lax.all_to_all(value, axes, split_axis=0, concat_axis=0, tiled=True)


def local(img_feat, txt_feat, w_img, w_txt, pair_index, log_scale, bias):
    x, y, z = (lax.axis_index(a) for a in (X, "y", Z))
    m = lax.axis_index(MP)
    octet = 4 * x + y
    where = jnp.stack([octet, z, m, y]).astype(jnp.int32)

    sent, *chosen = call(
        pack,
        (jax.ShapeDtypeStruct((32, 56, 128), bf16),)
        + (jax.ShapeDtypeStruct((32, 384), bf16),) * 4,
        [pltpu.VMEM((12, 288), bf16)] * 2
        + [pltpu.VMEM((16, 1536), bf16)] * 2
        + [pltpu.VMEM((8, 56, 128), bf16), pltpu.VMEM((4, 32, 384), bf16)]
        + [pltpu.SemaphoreType.DMA((4,)), pltpu.SemaphoreType.DMA((8,))],
        w_img,
        w_txt,
        img_feat,
        txt_feat,
        hbm=(0, 1, 2, 3),
        out=pltpu.HBM,
        vmem=60,
    )
    weights = exchange(sent, SPREAD)

    received = [chosen[0]]
    for k in range(1, 4):
        received.append(
            lax.ppermute(chosen[k], "y", [(s, (s + k) % 4) for s in range(4)])
        )

    sort, split, pairs, codes, scalars = call(
        setup,
        (
            jax.ShapeDtypeStruct((384, 384), bf16),
            jax.ShapeDtypeStruct((384, 128), bf16),
            jax.ShapeDtypeStruct((16, 128), jnp.int32),
            jax.ShapeDtypeStruct((8, 128), f32),
            jax.ShapeDtypeStruct((16, 128), f32),
        ),
        [],
        where,
        pair_index,
        log_scale,
        bias,
        smem=(0, 1, 2, 3),
    )

    sent = call(
        project,
        jax.ShapeDtypeStruct((8, 72, 128), bf16),
        [pltpu.VMEM((4, 32, 384), bf16)],
        where,
        sort,
        split,
        weights,
        *received,
        smem=(0,),
    )
    got = exchange(sent, ("y", "m0"))
    half = call(combine, jax.ShapeDtypeStruct((2, 72, 128), f32), [], got)
    got = lax.all_gather(half, "m1", axis=0, tiled=True)
    own = call(embed, jax.ShapeDtypeStruct((296, 128), bf16), [], got, codes)

    moves = []
    for s in range(512):
        o, rest = divmod(s, 32)
        moves.append((s, 32 * ((o - DELTA[rest % 4]) % 16) + rest))
    other = lax.ppermute(own, BATCH + MP, moves)
    sent = call(
        choose,
        jax.ShapeDtypeStruct((8, 296, 128), bf16),
        [pltpu.VMEM((2, 296, 128), bf16)],
        where,
        own,
        other,
        smem=(0,),
    )
    got = exchange(sent, Z_ORDER)
    sent = call(
        score,
        jax.ShapeDtypeStruct((4, 72, 128), bf16),
        [],
        where,
        scalars,
        pairs,
        own,
        got,
        smem=(0,),
    )
    got = exchange(sent, MP)
    return call(
        finish,
        (jax.ShapeDtypeStruct((16, 288), f32), jax.ShapeDtypeStruct((4, 1152), f32)),
        [],
        got,
    )


def solution(mesh):
    finer = Mesh(mesh.devices.reshape(2, 2, 4, 2, 2, 2, 2, 2), BATCH + MP)
    in_specs = (P(BATCH, None), P(BATCH, None), P(BATCH, MP), P(BATCH, MP), P(BATCH), P(), P())
    out_specs = (P(BATCH, MP), P(BATCH + MP, None))

    return jax.shard_map(local, mesh=finer, in_specs=in_specs, out_specs=out_specs, check_vma=False)
```
